128 devices in a mesh: grp: 8 (over z, core), dev: 16 (over x, y).
Axes of the slice: x: 4, y: 4, z: 4, core: 2. Of those that a mesh axis runs over, the one named last changes fastest.
Arguments:
- candidates: bfloat16 [262144, 512], P(('grp', 'dev')), may hold values from -6 to 6
- prefix_keys: bfloat16 [128, 1024, 512], P(('grp', 'dev')), may hold values from -6 to 6
- prefix_values: bfloat16 [128, 1024, 512], P(('grp', 'dev')), may hold values from -6 to 6
- cand_count: int32 [128], P(('grp', 'dev')), may hold values from 128 to 2048, as said below
- prefix_len: int32 [128], P(('grp', 'dev')), may hold values from 128 to 1024, as said below
- dest_device: int32 [2048], P(('grp', 'dev')), may hold values from 0 to 127, as said below
- dest_slot: int32 [2048], P(('grp', 'dev')), may hold values from 0 to 15, as said below
- norm_gain: float32 [512], replicated, may hold values from 0.5 to 1.5
- w_in: bfloat16 [512, 2048], replicated, may hold values from -0.25 to 0.25
- b_in: float32 [2048], replicated, may hold values from -3 to 3
- attn_gain: float32 [512], replicated, may hold values from 0.5 to 1.5
- w_out: bfloat16 [512, 512], replicated, may hold values from -0.25 to 0.25
Outputs:
- owned_blocks: bfloat16 [262144, 512], P(('grp', 'dev'))
The draws below stay inside these ranges and needn't reach their ends.
Inputs may be any that keep to these rules, and one draw needn't show every extreme that they name: `cand_count`: some user reaches the largest count in every draw. `prefix_len`: some user reaches the largest length in every draw. `dest_device`: devices are numbered in the order grp then dev. The 16 blocks of one device go to distinct devices, 2 of them to each index of grp and 1 to each index of dev. For every index of dev, the blocks that the devices with that index send to one index of grp go 1 to each index of dev. For every index of grp, the blocks that the devices with that index send to one index of dev go 2 to each index of grp. Every device receives exactly 16 blocks. `dest_slot`: the blocks that one device receives fill its 16 block offsets once each.
All inputs are finite; a program needn't handle non-finite values.
Results may differ from the reference program's by a relative error of at most 0.0057.
Values may be sent and summed in bfloat16 or wider, within the bound.
A program may use at most 128 MiB of HBM per device.

```python
import jax
import jax.numpy as jnp
from jax import lax

D = 512
HEADS = 4
BLK = 128
CBLK = 16
PMAX = 1024
BPD = 16
USERS = 128
N_GRP = 8
N_DEV = 16


def draw_cand_count(key, part):
    largest = CBLK * BLK
    draw_key, pick_key = jax.random.split(jax.random.fold_in(key, 3))
    counts = jax.random.randint(draw_key, (USERS,), largest // 16, largest + 1, dtype=jnp.int32)
    chosen = jax.random.randint(pick_key, (), 0, USERS, dtype=jnp.int32)
    return counts.at[chosen].set(largest)


def draw_prefix_len(key, part):
    largest = PMAX
    draw_key, pick_key = jax.random.split(jax.random.fold_in(key, 5))
    lengths = jax.random.randint(draw_key, (USERS,), largest // 8, largest + 1, dtype=jnp.int32)
    chosen = jax.random.randint(pick_key, (), 0, USERS, dtype=jnp.int32)
    return lengths.at[chosen].set(largest)


def route_table(key):
    folded = jax.random.fold_in(key, 11)
    subkeys = jax.random.split(folded, 6)
    grp_perm = jax.random.permutation(subkeys[0], N_GRP)
    grp_shift = jax.random.permutation(subkeys[1], N_GRP)
    dev_perm = jax.random.permutation(subkeys[2], N_DEV)
    dev_shift = jax.random.permutation(subkeys[3], N_DEV)
    shuffled = jax.random.permutation(subkeys[4], BPD)
    per_group = BPD // N_GRP
    grp_offset = shuffled // per_group
    dev_offset = shuffled % N_DEV
    source = jnp.arange(N_GRP * N_DEV, dtype=jnp.int32)
    src_group = source // N_DEV
    src_member = source % N_DEV
    target_group = grp_perm[(grp_shift[src_group][:, None] + grp_offset[None, :]) % N_GRP]
    target_member = dev_perm[(dev_shift[src_member][:, None] + dev_offset[None, :]) % N_DEV]
    target = target_group * N_DEV + target_member
    slot_keys = jax.random.split(subkeys[5], N_GRP * N_DEV)
    slot_table = jax.vmap(lambda slot_key: jax.random.permutation(slot_key, BPD))(slot_keys)
    slot_ids = slot_table[target, jnp.arange(BPD)[None, :]]
    return (target.reshape(-1).astype(jnp.int32), slot_ids.reshape(-1).astype(jnp.int32))


def draw_dest_device(key, part):
    return route_table(key)[0]


def draw_dest_slot(key, part):
    return route_table(key)[1]


def block_scale(key, dims, shards, smallest, top_value):
    def one(dim, blocks):
        steps = jax.random.uniform(jax.random.fold_in(jax.random.fold_in(key, 6), dim), (blocks,), jnp.float32, smallest / len(shards), top_value / len(shards))
        return jnp.repeat(jnp.exp(steps), dims[dim] // blocks).reshape((-1,) + (1,) * (len(dims) - dim - 1))

    factor_of = one(*shards[0])
    for cut in shards[1:]:
        factor_of = factor_of * one(*cut)
    return factor_of


def noise(rng, shape, scale, most, cuts=(), kind=jnp.bfloat16):
    level = block_scale(rng, shape, cuts, -0.22, 0.18) if cuts else 1.0
    values = jax.random.normal(rng, shape, jnp.float32) * scale * level
    return jnp.minimum(jnp.maximum(values, -most), most).astype(kind)


def setup_inputs(seed: int = 0) -> dict:
    arg_keys = jax.random.split(jax.random.key(seed), 13)
    candidates = noise(arg_keys[0], (USERS * CBLK * BLK, D), 1.0, 6.0, ((0, 128),))
    prefix_keys = noise(arg_keys[1], (USERS, PMAX, D), 1.0, 6.0, ((0, 128),))
    prefix_values = noise(arg_keys[2], (USERS, PMAX, D), 1.0, 6.0, ((0, 128),))
    cand_count = draw_cand_count(jax.random.fold_in(arg_keys[12], 71), 0)
    prefix_len = draw_prefix_len(jax.random.fold_in(arg_keys[12], 71), 0)
    dest_device = draw_dest_device(jax.random.fold_in(arg_keys[12], 71), 0)
    dest_slot = draw_dest_slot(jax.random.fold_in(arg_keys[12], 71), 0)
    norm_gain = jnp.clip(1.0 + 0.1 * jax.random.normal(arg_keys[7], (D,), jnp.float32), 0.5, 1.5)
    w_in = noise(arg_keys[8], (D, 4 * D), D ** -0.5, 0.25)
    b_in = noise(arg_keys[9], (4 * D,), 0.5, 3.0, (), jnp.float32)
    attn_gain = jnp.clip(1.0 + 0.1 * jax.random.normal(arg_keys[10], (D,), jnp.float32), 0.5, 1.5)
    w_out = noise(arg_keys[11], (D, D), D ** -0.5, 0.25)
    return dict(candidates=candidates, prefix_keys=prefix_keys, prefix_values=prefix_values, cand_count=cand_count, prefix_len=prefix_len, dest_device=dest_device, dest_slot=dest_slot, norm_gain=norm_gain, w_in=w_in, b_in=b_in, attn_gain=attn_gain, w_out=w_out)


def normalize(matrix, gain):
    average = lax.optimization_barrier(jnp.mean(matrix, axis=-1, keepdims=True))
    centred = matrix - average
    spread = lax.optimization_barrier(jnp.mean(centred * centred, axis=-1, keepdims=True))
    return centred * lax.rsqrt(spread + 1e-06) * gain

def user_output(cand_rows, key_rows, value_rows, live_count, length, norm_gain, w_in, b_in, attn_gain, w_out):
    row_total = cand_rows.shape[0]
    model_width = cand_rows.shape[1]
    head_dim = model_width // HEADS
    scale = 1.0 / jnp.sqrt(jnp.float32(head_dim))
    inputs_f = cand_rows.astype(jnp.float32)
    normed = normalize(inputs_f, norm_gain).astype(jnp.bfloat16)
    projected = jax.nn.silu(jnp.dot(normed, w_in, preferred_element_type=jnp.float32) + b_in).astype(jnp.bfloat16)
    gate_part, value_part, query_part, key_part = jnp.split(projected, 4, axis=1)
    queries = query_part.reshape(row_total, HEADS, head_dim).astype(jnp.float32)
    own_keys = key_part.reshape(row_total, HEADS, head_dim).astype(jnp.float32)
    own_values = value_part.reshape(row_total, HEADS, head_dim).astype(jnp.float32)
    prefix_k = key_rows.reshape(-1, HEADS, head_dim).astype(jnp.float32)
    prefix_v = value_rows.reshape(-1, HEADS, head_dim).astype(jnp.float32)
    scores = jnp.einsum('rhd,jhd->hrj', queries, prefix_k) * scale
    key_live = jnp.arange(prefix_k.shape[0], dtype=jnp.int32) < length
    weights = jnp.where(key_live[None, None, :], jax.nn.silu(scores), 0.0).astype(jnp.bfloat16)
    self_weight = jax.nn.silu(lax.optimization_barrier(jnp.sum(queries * own_keys, axis=-1)) * scale).astype(jnp.bfloat16)
    attended = jnp.einsum('hrj,jhd->rhd', weights.astype(jnp.float32), prefix_v)
    attended = attended + self_weight.astype(jnp.float32)[:, :, None] * own_values
    attended = attended.reshape(row_total, model_width)
    gated_rows = (normalize(attended, attn_gain) * gate_part.astype(jnp.float32)).astype(jnp.bfloat16)
    layer_out = inputs_f + jnp.dot(gated_rows, w_out, preferred_element_type=jnp.float32)
    live_rows = jnp.arange(row_total, dtype=jnp.int32) < live_count
    return jnp.where(live_rows[:, None], layer_out, 0.0).astype(jnp.bfloat16)

def reference(candidates, prefix_keys, prefix_values, cand_count, prefix_len, dest_device, dest_slot, norm_gain, w_in, b_in, attn_gain, w_out):
    per_user = CBLK * BLK

    def one_user(inputs):
        cand_rows, key_rows, value_rows, live_count, length = inputs
        return user_output(cand_rows, key_rows, value_rows, live_count, length, norm_gain, w_in, b_in, attn_gain, w_out)
    outputs = lax.map(one_user, (candidates.reshape(USERS, per_user, D), prefix_keys, prefix_values, cand_count, prefix_len))
    blocks = outputs.reshape(USERS * CBLK, BLK, D)
    placed = (dest_device * BPD + dest_slot).astype(jnp.int32)
    inverse = jnp.zeros((USERS * CBLK,), jnp.int32).at[placed].set(jnp.arange(USERS * CBLK, dtype=jnp.int32))
    return blocks[inverse].reshape(USERS * CBLK * BLK, D)
```

```python
import functools

import jax
import jax.numpy as jnp
from jax import lax
from jax.experimental import pallas as pl
from jax.experimental.pallas import tpu as pltpu
from jax.sharding import PartitionSpec as P

HEADS = 4
BLK = 128
CHUNKS = 4
KEY_TILE = 256
MESH = pl.DeviceIdType.MESH
F32 = jnp.float32
BF16 = jnp.bfloat16
ORDER_G, ORDER_D, PICK_1, PICK_2, SLOT_1, SLOT_2 = range(6)


def log2(number):
    return number.bit_length() - 1


def lanes(shape):
    return lax.broadcasted_iota(jnp.int32, shape, 1)


def rows_of(shape):
    return lax.broadcasted_iota(jnp.int32, shape, 0)


def stack_rows(ref, count):
    tiles = []
    for first in range(0, count, 8):
        tile = jnp.full((8, 128), -1, jnp.int32)
        for step in range(first, min(first + 8, count)):
            tile = jnp.where(rows_of((8, 128)) == step - first, ref[step], tile)
        tiles.append(tile)
    return tiles[0] if len(tiles) == 1 else jnp.concatenate(tiles, axis=0)


def column(matrix, index):
    return matrix[:, index : index + 1]


def centre(matrix, width):
    average = jnp.sum(matrix, axis=-1, keepdims=True) * (1.0 / width)
    centred = matrix - average
    spread = jnp.sum(centred * centred, axis=-1, keepdims=True) * (1.0 / width)
    return centred * lax.rsqrt(spread + 1e-06)


def half_silu(half):
    return half + half * jnp.tanh(half)


def kernel(sizes, *refs):
    ng, nd, nblk, width, prefix, rows = sizes
    piece = BLK // CHUNKS
    part = piece // 2
    sub = nblk // 2
    tile_rows = sub * piece
    head_dim = width // HEADS
    (
        count_ref,
        length_ref,
        device_ref,
        slot_ref,
        gain_ref,
        bias_ref,
        again_ref,
        cand_hbm,
        key_hbm,
        value_hbm,
        win_hbm,
        wout_hbm,
        out_ref,
        cand,
        keys,
        keys_t,
        values,
        win,
        wout,
        proj,
        res,
        tab_own,
        tab_g,
        tab_d,
        slot_own_1,
        slot_own_2,
        slot_in_1,
        slot_in_2,
        idx_v,
        idx,
        load_sem,
        idx_sem,
        meta_send,
        meta_recv,
        data_send,
        data_recv,
        *bufs,
    ) = refs
    send_a1, recv_a1, send_b1, recv_b1, send_a2, recv_a2, send_b2, recv_b2 = (
        bufs[CHUNKS * k : CHUNKS * (k + 1)] for k in range(8)
    )
    me_g = lax.axis_index("grp")
    me_d = lax.axis_index("dev")

    def at_group(step):
        return {"grp": (me_g + step) & (ng - 1), "dev": me_d}

    def at_member(step):
        return {"grp": me_g, "dev": (me_d + step) & (nd - 1)}

    loads = [
        pltpu.make_async_copy(src, dst, load_sem.at[k])
        for k, (src, dst) in enumerate(
            (
                (cand_hbm, cand),
                (win_hbm, win),
                (key_hbm, keys),
                (value_hbm, values),
                (wout_hbm, wout),
            )
        )
    ]
    for load in loads:
        load.start()

    barrier = pltpu.get_barrier_semaphore()

    def greet_group(step, carry):
        pl.semaphore_signal(barrier, inc=1, device_id=at_group(step), device_id_type=MESH)
        return carry

    def greet_member(step, carry):
        pl.semaphore_signal(barrier, inc=1, device_id=at_member(step), device_id_type=MESH)
        return carry

    lax.fori_loop(1, ng, greet_group, 0)
    lax.fori_loop(1, nd, greet_member, 0)

    def own_table():
        tab_own[...] = jnp.full((8, 128), -1, jnp.int32)
        code = device_ref[...] * nblk + slot_ref[...]
        tab_own[:, 0:nblk] = jnp.broadcast_to(code, (8, nblk))
        table = tab_own[...]
        device = lax.shift_right_arithmetic(table, log2(nblk))
        group = lax.shift_right_arithmetic(device, log2(nd))
        member = jnp.where(table < 0, -1, device & (nd - 1))
        lane = lanes((8, 128))
        live = lane < nblk
        want_g = jnp.where(
            live, (me_g + lax.shift_right_arithmetic(lane, 1)) & (ng - 1), -7
        )
        want_d = jnp.where(live, (me_d + lane) & (nd - 1), -7)
        low = jnp.full((8, 128), nblk - 1, jnp.int32)
        high = jnp.zeros((8, 128), jnp.int32)
        order_d = jnp.zeros((8, 128), jnp.int32)
        for i in range(nblk):
            hit_g = column(group, i) == want_g
            low = jnp.where(hit_g, jnp.minimum(low, i), low)
            high = jnp.where(hit_g, jnp.maximum(high, i), high)
            order_d = jnp.where(column(member, i) == want_d, i, order_d)
        order_g = jnp.where((lane & 1) == 0, low, high)
        row = rows_of((8, 128))
        idx_v[...] = jnp.where(
            row == ORDER_G, order_g, jnp.where(row == ORDER_D, order_d, 0)
        )
        tab_g[0] = table
        tab_d[0] = table

    def publish():
        copy = pltpu.make_async_copy(idx_v, idx, idx_sem)
        copy.start()
        copy.wait()

    def send_tables():
        def to_group(step, carry):
            pltpu.make_async_remote_copy(
                tab_own, tab_g.at[step], meta_send.at[0], meta_recv.at[0], at_group(step), MESH
            ).start()
            return carry

        def to_member(step, carry):
            pltpu.make_async_remote_copy(
                tab_own, tab_d.at[step], meta_send.at[1], meta_recv.at[1], at_member(step), MESH
            ).start()
            return carry

        lax.fori_loop(1, ng, to_group, 0)
        lax.fori_loop(1, nd, to_member, 0)

    def wait_bytes(sem, ref):
        pltpu.make_async_copy(ref, ref, sem).wait()

    def middle_tables():
        wait_bytes(meta_recv.at[0], tab_g.at[pl.ds(1, ng - 1)])
        wait_bytes(meta_recv.at[1], tab_d.at[pl.ds(1, nd - 1)])
        table = stack_rows(tab_g, ng)
        shape = table.shape
        device = lax.shift_right_arithmetic(table, log2(nblk))
        group = lax.shift_right_arithmetic(device, log2(nd))
        slot = table & (nblk - 1)
        lane = lanes(shape)
        mine = group == me_g
        first = jnp.min(
            jnp.where(mine, lane.astype(F32), 1000.0), axis=1, keepdims=True
        ).astype(jnp.int32)
        place = 2 * rows_of(shape) + jnp.where(lane > first, 1, 0)
        both = place * nblk + slot
        want = jnp.where(lane < nblk, me_g * nd + ((me_d + lane) & (nd - 1)), -7)
        found = jnp.zeros(shape, jnp.int32)
        for i in range(nblk):
            found = found + jnp.where(column(device, i) == want, column(both, i), 0)
        found = jnp.sum(found, axis=0, keepdims=True)
        found = jnp.broadcast_to(found, (8, 128))
        pick_1 = lax.shift_right_arithmetic(found, log2(nblk))
        slot_own_1[...] = found & (nblk - 1)
        table = stack_rows(tab_d, nd)
        shape = table.shape
        device = lax.shift_right_arithmetic(table, log2(nblk))
        both = rows_of(shape) * nblk + (table & (nblk - 1))
        lane = lanes(shape)
        want = jnp.where(
            lane < nblk,
            ((me_g + lax.shift_right_arithmetic(lane, 1)) & (ng - 1)) * nd + me_d,
            -7,
        )
        top = nd * nblk - 1
        low = jnp.full(shape, top, jnp.int32)
        high = jnp.zeros(shape, jnp.int32)
        for i in range(nblk):
            hit = column(device, i) == want
            low = jnp.where(hit, jnp.minimum(low, column(both, i)), low)
            high = jnp.where(hit, jnp.maximum(high, column(both, i)), high)
        low = jnp.broadcast_to(jnp.min(low, axis=0, keepdims=True), (8, 128))
        high = jnp.broadcast_to(jnp.max(high, axis=0, keepdims=True), (8, 128))
        found = jnp.where((lanes((8, 128)) & 1) == 0, low, high)
        pick_2 = lax.shift_right_arithmetic(found, log2(nblk))
        slot_own_2[...] = found & (nblk - 1)
        row = rows_of((8, 128))
        idx_v[...] = jnp.where(
            row == PICK_1, pick_1, jnp.where(row == PICK_2, pick_2, idx_v[...])
        )
        slot_in_1[0] = slot_own_1[...]
        slot_in_2[0] = slot_own_2[...]

        def to_member(step, carry):
            pltpu.make_async_remote_copy(
                slot_own_1, slot_in_1.at[step], meta_send.at[2], meta_recv.at[2],
                at_member(step), MESH,
            ).start()
            return carry

        def to_group(step, carry):
            pltpu.make_async_remote_copy(
                slot_own_2, slot_in_2.at[step], meta_send.at[3], meta_recv.at[3],
                at_group(step), MESH,
            ).start()
            return carry

        lax.fori_loop(1, nd, to_member, 0)
        lax.fori_loop(1, ng, to_group, 0)
        publish()

    def final_tables():
        wait_bytes(meta_recv.at[2], slot_in_1.at[pl.ds(1, nd - 1)])
        wait_bytes(meta_recv.at[3], slot_in_2.at[pl.ds(1, ng - 1)])

        def place(table, lane_of_row, number):
            lane, row = lanes(table.shape), rows_of(table.shape)
            slot = jnp.sum(
                jnp.where(lane == lane_of_row(row), table, 0).astype(F32), axis=1, keepdims=True
            ).astype(jnp.int32)
            slot = jnp.where(column(row, 0) < number, slot, -7)
            hit = jnp.where(slot == lane, lane_of_row(row), 0)
            return jnp.broadcast_to(jnp.sum(hit, axis=0, keepdims=True), (8, 128))

        table = stack_rows(slot_in_1, nd)
        slot_1 = place(table, lambda row: row, nd)
        table = stack_rows(slot_in_2, ng)
        slot_2 = place(table, lambda row: 2 * row, ng) + place(table, lambda row: 2 * row + 1, ng)
        row = rows_of((8, 128))
        idx_v[...] = jnp.where(
            row == SLOT_1, slot_1, jnp.where(row == SLOT_2, slot_2, idx_v[...])
        )
        publish()

    def look(row, lane):
        return idx[row, lane] & (nblk - 1)

    def remote(src, dst, kind, c, where):
        return pltpu.make_async_remote_copy(
            src, dst, data_send.at[kind, c], data_recv.at[kind, c], where, MESH
        )

    def send_first(c):
        for k in range(2):
            recv_a1[c][k] = res[look(ORDER_G, k), 0:part, :]
        recv_a2[c][0] = res[look(ORDER_D, 0), part:piece, :]

        def group_step(step, carry):
            for k in range(2):
                send_a1[c][2 * step + k] = res[look(ORDER_G, 2 * step + k), 0:part, :]
            span = pl.ds(2 * step, 2)
            remote(send_a1[c].at[span], recv_a1[c].at[span], 0, c, at_group(step)).start()
            return carry

        def member_step(step, carry):
            send_a2[c][step] = res[look(ORDER_D, step), part:piece, :]
            remote(send_a2[c].at[step], recv_a2[c].at[step], 1, c, at_member(step)).start()
            return carry

        lax.fori_loop(1, ng, group_step, 0)
        lax.fori_loop(1, nd, member_step, 0)

    def send_second(c):
        wait_bytes(data_recv.at[0, c], recv_a1[c].at[pl.ds(2, nblk - 2)])
        recv_b1[c][0] = recv_a1[c][look(PICK_1, 0)]

        def member_step(step, carry):
            send_b1[c][step] = recv_a1[c][look(PICK_1, step)]
            remote(send_b1[c].at[step], recv_b1[c].at[step], 2, c, at_member(step)).start()
            return carry

        lax.fori_loop(1, nd, member_step, 0)
        wait_bytes(data_recv.at[1, c], recv_a2[c].at[pl.ds(1, nd - 1)])
        for k in range(2):
            recv_b2[c][k] = recv_a2[c][look(PICK_2, k)]

        def group_step(step, carry):
            for k in range(2):
                send_b2[c][2 * step + k] = recv_a2[c][look(PICK_2, 2 * step + k)]
            span = pl.ds(2 * step, 2)
            remote(send_b2[c].at[span], recv_b2[c].at[span], 3, c, at_group(step)).start()
            return carry

        lax.fori_loop(1, ng, group_step, 0)

    def deliver(c):
        wait_bytes(data_recv.at[2, c], recv_b1[c].at[pl.ds(1, nd - 1)])
        wait_bytes(data_recv.at[3, c], recv_b2[c].at[pl.ds(2, nblk - 2)])

        def slot_step(s, carry):
            out_ref[s, c * piece : c * piece + part, :] = recv_b1[c][look(SLOT_1, s)]
            out_ref[s, c * piece + part : (c + 1) * piece, :] = recv_b2[c][look(SLOT_2, s)]
            return carry

        lax.fori_loop(0, nblk, slot_step, 0)

    def prepare_prefix():
        loads[2].wait()
        loads[3].wait()
        live = length_ref[0]
        for first in range(0, prefix, KEY_TILE):
            span = slice(first, first + KEY_TILE)
            keys_t[:, span] = keys[span, :].T
            shape = (KEY_TILE, width)
            values[span, :] = jnp.where(
                rows_of(shape) + first < live, values[span, :], jnp.zeros(shape, BF16)
            )

    score_scale = 0.5 / (head_dim**0.5)

    def compute(t):
        c = lax.shift_right_logical(t, 1)
        first_block = pl.multiple_of((t & 1) * sub, sub)
        first_row = pl.multiple_of(c * piece, piece)

        @pl.when(t == 0)
        def _():
            loads[0].wait()
            loads[1].wait()

        x = cand[pl.ds(first_block, sub), pl.ds(first_row, piece), :]
        x = x.reshape(tile_rows, width).astype(F32)
        normed = (centre(x, width) * (gain_ref[...] * 0.5)).astype(BF16)
        step_cols = 256
        for first in range(0, 4 * width, step_cols):
            span = slice(first, first + step_cols)
            half = jnp.dot(normed, win[:, span], preferred_element_type=F32)
            act = half_silu(half + bias_ref[:, span] * 0.5)
            if 2 * width <= first < 3 * width:
                act = act * score_scale
            proj[:, span] = act.astype(BF16)

        @pl.when(t == 0)
        def _():
            prepare_prefix()
            loads[4].wait()

        heads = []
        for h in range(HEADS):
            cols = slice(h * head_dim, (h + 1) * head_dim)
            query = proj[:, 2 * width + h * head_dim : 2 * width + (h + 1) * head_dim]
            own_key = proj[:, 3 * width + h * head_dim : 3 * width + (h + 1) * head_dim]
            own_value = proj[:, width + h * head_dim : width + (h + 1) * head_dim]
            total = None
            for first in range(0, prefix, KEY_TILE):
                span = slice(first, first + KEY_TILE)
                half = jnp.dot(query, keys_t[cols, span], preferred_element_type=F32)
                weights = half_silu(half).astype(BF16)
                term = jnp.dot(weights, values[span, cols], preferred_element_type=F32)
                total = term if total is None else total + term
            own = jnp.sum(query.astype(F32) * own_key.astype(F32), axis=-1, keepdims=True)
            own = half_silu(own).astype(BF16).astype(F32)
            heads.append(total + own * own_value.astype(F32))
        attended = jnp.concatenate(heads, axis=1)
        gated = (
            centre(attended, width) * again_ref[...] * proj[:, 0:width].astype(F32)
        ).astype(BF16)
        x = cand[pl.ds(first_block, sub), pl.ds(first_row, piece), :]
        x = x.reshape(tile_rows, width).astype(F32)
        layer_out = x + jnp.dot(gated, wout[...], preferred_element_type=F32)
        shape = (sub, piece, width)
        row = (
            (lax.broadcasted_iota(jnp.int32, shape, 0) + first_block) * BLK
            + lax.broadcasted_iota(jnp.int32, shape, 1)
            + first_row
        )
        layer_out = jnp.where(row < count_ref[0], layer_out.reshape(shape), 0.0)
        res[pl.ds(first_block, sub), :, :] = layer_out.astype(BF16)

    own_table()
    publish()

    def step(t, carry):
        compute(t)

        @pl.when(t == 0)
        def _():
            pl.semaphore_wait(barrier, ng + nd - 2)
            send_tables()

        for c in range(CHUNKS):

            @pl.when(t == 2 * c + 1)
            def _():
                send_first(c)
                if c == 1:
                    middle_tables()
                if c >= 1:
                    send_second(c - 1)
                if c == 2:
                    final_tables()
                if c >= 2:
                    deliver(c - 2)

        return carry

    lax.fori_loop(0, 2 * CHUNKS, step, 0)
    last = CHUNKS - 1
    send_second(last)
    deliver(last - 1)
    deliver(last)

    wait_bytes(meta_send.at[0], tab_g.at[pl.ds(1, ng - 1)])
    wait_bytes(meta_send.at[1], tab_d.at[pl.ds(1, nd - 1)])
    wait_bytes(meta_send.at[2], slot_in_1.at[pl.ds(1, nd - 1)])
    wait_bytes(meta_send.at[3], slot_in_2.at[pl.ds(1, ng - 1)])
    for c in range(CHUNKS):
        wait_bytes(data_send.at[0, c], send_a1[c].at[pl.ds(2, nblk - 2)])
        wait_bytes(data_send.at[1, c], send_a2[c].at[pl.ds(1, nd - 1)])
        wait_bytes(data_send.at[2, c], send_b1[c].at[pl.ds(1, nd - 1)])
        wait_bytes(data_send.at[3, c], send_b2[c].at[pl.ds(2, nblk - 2)])


def layer(
    ng,
    nd,
    candidates,
    prefix_keys,
    prefix_values,
    cand_count,
    prefix_len,
    dest_device,
    dest_slot,
    norm_gain,
    w_in,
    b_in,
    attn_gain,
    w_out,
):
    rows, width = candidates.shape
    prefix = prefix_keys.shape[1]
    nblk = rows // BLK
    part = BLK // CHUNKS // 2
    tile_rows = nblk // 2 * (BLK // CHUNKS)
    smem = pl.BlockSpec(memory_space=pltpu.SMEM)
    vmem = pl.BlockSpec(memory_space=pltpu.VMEM)
    hbm = pl.BlockSpec(memory_space=pl.ANY)
    block = pltpu.VMEM((nblk, part, width), BF16)
    table = pltpu.VMEM((8, 128), jnp.int32)
    out = pl.pallas_call(
        functools.partial(kernel, (ng, nd, nblk, width, prefix, rows)),
        out_shape=jax.ShapeDtypeStruct((nblk, BLK, width), BF16),
        in_specs=[smem, smem, vmem, vmem, vmem, vmem, vmem, hbm, hbm, hbm, hbm, hbm],
        out_specs=vmem,
        scratch_shapes=[
            pltpu.VMEM((nblk, BLK, width), BF16),
            pltpu.VMEM((prefix, width), BF16),
            pltpu.VMEM((width, prefix), BF16),
            pltpu.VMEM((prefix, width), BF16),
            pltpu.VMEM((width, 4 * width), BF16),
            pltpu.VMEM((width, width), BF16),
            pltpu.VMEM((tile_rows, 4 * width), BF16),
            pltpu.VMEM((nblk, BLK // CHUNKS, width), BF16),
            table,
            pltpu.VMEM((ng, 8, 128), jnp.int32),
            pltpu.VMEM((nd, 8, 128), jnp.int32),
            table,
            table,
            pltpu.VMEM((nd, 8, 128), jnp.int32),
            pltpu.VMEM((ng, 8, 128), jnp.int32),
            table,
            pltpu.SMEM((8, 128), jnp.int32),
            pltpu.SemaphoreType.DMA((5,)),
            pltpu.SemaphoreType.DMA,
            pltpu.SemaphoreType.DMA((4,)),
            pltpu.SemaphoreType.DMA((4,)),
            pltpu.SemaphoreType.DMA((4, CHUNKS)),
            pltpu.SemaphoreType.DMA((4, CHUNKS)),
        ]
        + [block] * (8 * CHUNKS),
        compiler_params=pltpu.CompilerParams(
            collective_id=0, has_side_effects=True, vmem_limit_bytes=60 * 2**20
        ),
    )(
        cand_count,
        prefix_len,
        dest_device.reshape(1, nblk),
        dest_slot.reshape(1, nblk),
        norm_gain.reshape(1, width),
        b_in.reshape(1, 4 * width),
        attn_gain.reshape(1, width),
        candidates.reshape(nblk, BLK, width),
        prefix_keys[0],
        prefix_values[0],
        w_in,
        w_out,
    )
    return out.reshape(rows, width)


def solution(mesh):
    spec = P(("grp", "dev"))
    wide = P(("grp", "dev"), None)
    deep = P(("grp", "dev"), None, None)
    return jax.shard_map(
        functools.partial(layer, mesh.shape["grp"], mesh.shape["dev"]),
        mesh=mesh,
        in_specs=(wide, deep, deep, spec, spec, spec, spec, P(), P(), P(), P(), P()),
        out_specs=wide,
        check_vma=False,
    )
```

```python
import functools

import jax
import jax.numpy as jnp
from jax import lax
from jax.experimental import pallas as pl
from jax.experimental.pallas import tpu as pltpu
from jax.sharding import PartitionSpec as P

HEADS = 4
BLK = 128
CHUNKS = 8
LAG = 4
LAST_LAG = 7
KEY_TILE = 256
AHEAD = 2
COLS = 256
MESH = pl.DeviceIdType.MESH
F32 = jnp.float32
BF16 = jnp.bfloat16
ORDER_G, ORDER_D, PICK_1, PICK_2, SLOT_1, SLOT_2 = range(6)


def log2(number):
    return number.bit_length() - 1


def lanes(shape):
    return lax.broadcasted_iota(jnp.int32, shape, 1)


def rows_of(shape):
    return lax.broadcasted_iota(jnp.int32, shape, 0)


def stack_rows(ref, count):
    tiles = []
    for first in range(0, count, 8):
        tile = jnp.full((8, 128), -1, jnp.int32)
        for step in range(first, min(first + 8, count)):
            tile = jnp.where(rows_of((8, 128)) == step - first, ref[step], tile)
        tiles.append(tile)
    return tiles[0] if len(tiles) == 1 else jnp.concatenate(tiles, axis=0)


def column(matrix, index):
    return matrix[:, index : index + 1]


def centre(matrix, width):
    average = jnp.sum(matrix, axis=-1, keepdims=True) * (1.0 / width)
    centred = matrix - average
    spread = jnp.sum(centred * centred, axis=-1, keepdims=True) * (1.0 / width)
    return centred * lax.rsqrt(spread + 1e-06)


def half_silu(half):
    return half + half * jnp.tanh(half)


def kernel(sizes, *refs):
    ng, nd, nblk, width, prefix = sizes
    piece = BLK // CHUNKS
    tile_rows = nblk * piece
    head_dim = width // HEADS
    (
        count_hbm,
        length_hbm,
        device_hbm,
        slot_hbm,
        gain_hbm,
        bias_hbm,
        again_hbm,
        cand_hbm,
        key_hbm,
        value_hbm,
        win_hbm,
        wout_hbm,
        out_ref,
        count_ref,
        length_ref,
        device_ref,
        slot_ref,
        gain_ref,
        bias_ref,
        again_ref,
        cand_first,
        cand,
        keys,
        keys_t,
        values,
        win,
        wout,
        nrm,
        gate,
        qkv,
        att,
        tab_own,
        tab_g,
        tab_d,
        slot_own_1,
        slot_own_2,
        slot_in_1,
        slot_in_2,
        idx_v,
        idx,
        load_sem,
        idx_sem,
        meta_send,
        meta_recv,
        data_send,
        data_recv,
        *bufs,
    ) = refs
    send_a, recv_a, send_b, recv_b = (bufs[CHUNKS * k : CHUNKS * (k + 1)] for k in range(4))
    me_g = lax.axis_index("grp")
    me_d = lax.axis_index("dev")

    def at_group(step):
        return {"grp": (me_g + step) & (ng - 1), "dev": me_d}

    def at_member(step):
        return {"grp": me_g, "dev": (me_d + step) & (nd - 1)}

    (
        load_device,
        load_slot,
        load_gain,
        load_bias,
        load_again,
        load_count,
        load_length,
        load_first,
        load_win,
        load_keys,
        load_values,
        load_cand,
        load_wout,
    ) = loads = [
        pltpu.make_async_copy(src, dst, load_sem.at[k])
        for k, (src, dst) in enumerate(
            (
                (device_hbm, device_ref),
                (slot_hbm, slot_ref),
                (gain_hbm, gain_ref),
                (bias_hbm, bias_ref),
                (again_hbm, again_ref),
                (count_hbm, count_ref),
                (length_hbm, length_ref),
                (cand_hbm.at[:, pl.ds(0, piece), :], cand_first),
                (win_hbm, win),
                (key_hbm, keys),
                (value_hbm, values),
                (cand_hbm, cand),
                (wout_hbm, wout),
            )
        )
    ]
    for load in loads:
        load.start()

    barrier = pltpu.get_barrier_semaphore()

    def greet_group(step, carry):
        pl.semaphore_signal(barrier, inc=1, device_id=at_group(step), device_id_type=MESH)
        return carry

    def greet_member(step, carry):
        pl.semaphore_signal(barrier, inc=1, device_id=at_member(step), device_id_type=MESH)
        return carry

    lax.fori_loop(1, ng, greet_group, 0)
    lax.fori_loop(1, nd, greet_member, 0)

    def own_table():
        tab_own[...] = jnp.full((8, 128), -1, jnp.int32)
        code = device_ref[...] * nblk + slot_ref[...]
        tab_own[:, 0:nblk] = jnp.broadcast_to(code, (8, nblk))
        table = tab_own[...]
        device = lax.shift_right_arithmetic(table, log2(nblk))
        group = lax.shift_right_arithmetic(device, log2(nd))
        member = jnp.where(table < 0, -1, device & (nd - 1))
        lane = lanes((8, 128))
        live = lane < nblk
        want_g = jnp.where(
            live, (me_g + lax.shift_right_arithmetic(lane, 1)) & (ng - 1), -7
        )
        want_d = jnp.where(live, (me_d + lane) & (nd - 1), -7)
        low = jnp.full((8, 128), nblk - 1, jnp.int32)
        high = jnp.zeros((8, 128), jnp.int32)
        order_d = jnp.zeros((8, 128), jnp.int32)
        for i in range(nblk):
            hit_g = column(group, i) == want_g
            low = jnp.where(hit_g, jnp.minimum(low, i), low)
            high = jnp.where(hit_g, jnp.maximum(high, i), high)
            order_d = jnp.where(column(member, i) == want_d, i, order_d)
        order_g = jnp.where((lane & 1) == 0, low, high)
        row = rows_of((8, 128))
        idx_v[...] = jnp.where(
            row == ORDER_G, order_g, jnp.where(row == ORDER_D, order_d, 0)
        )
        tab_g[0] = table
        tab_d[0] = table

    def publish():
        copy = pltpu.make_async_copy(idx_v, idx, idx_sem)
        copy.start()
        copy.wait()

    def send_tables():
        def to_group(step, carry):
            pltpu.make_async_remote_copy(
                tab_own, tab_g.at[step], meta_send.at[0], meta_recv.at[0], at_group(step), MESH
            ).start()
            return carry

        def to_member(step, carry):
            pltpu.make_async_remote_copy(
                tab_own, tab_d.at[step], meta_send.at[1], meta_recv.at[1], at_member(step), MESH
            ).start()
            return carry

        lax.fori_loop(1, ng, to_group, 0)
        lax.fori_loop(1, nd, to_member, 0)

    def wait_bytes(sem, ref):
        pltpu.make_async_copy(ref, ref, sem).wait()

    def middle_tables():
        wait_bytes(meta_recv.at[0], tab_g.at[pl.ds(1, ng - 1)])
        wait_bytes(meta_recv.at[1], tab_d.at[pl.ds(1, nd - 1)])
        table = stack_rows(tab_g, ng)
        shape = table.shape
        device = lax.shift_right_arithmetic(table, log2(nblk))
        group = lax.shift_right_arithmetic(device, log2(nd))
        slot = table & (nblk - 1)
        lane = lanes(shape)
        mine = group == me_g
        first = jnp.min(
            jnp.where(mine, lane.astype(F32), 1000.0), axis=1, keepdims=True
        ).astype(jnp.int32)
        place = 2 * rows_of(shape) + jnp.where(lane > first, 1, 0)
        both = place * nblk + slot
        want = jnp.where(lane < nblk, me_g * nd + ((me_d + lane) & (nd - 1)), -7)
        found = jnp.zeros(shape, jnp.int32)
        for i in range(nblk):
            found = found + jnp.where(column(device, i) == want, column(both, i), 0)
        found = jnp.sum(found, axis=0, keepdims=True)
        found = jnp.broadcast_to(found, (8, 128))
        pick_1 = lax.shift_right_arithmetic(found, log2(nblk))
        slot_own_1[...] = found & (nblk - 1)
        table = stack_rows(tab_d, nd)
        shape = table.shape
        device = lax.shift_right_arithmetic(table, log2(nblk))
        both = rows_of(shape) * nblk + (table & (nblk - 1))
        lane = lanes(shape)
        want = jnp.where(
            lane < nblk,
            ((me_g + lax.shift_right_arithmetic(lane, 1)) & (ng - 1)) * nd + me_d,
            -7,
        )
        top = nd * nblk - 1
        low = jnp.full(shape, top, jnp.int32)
        high = jnp.zeros(shape, jnp.int32)
        for i in range(nblk):
            hit = column(device, i) == want
            low = jnp.where(hit, jnp.minimum(low, column(both, i)), low)
            high = jnp.where(hit, jnp.maximum(high, column(both, i)), high)
        low = jnp.broadcast_to(jnp.min(low, axis=0, keepdims=True), (8, 128))
        high = jnp.broadcast_to(jnp.max(high, axis=0, keepdims=True), (8, 128))
        found = jnp.where((lanes((8, 128)) & 1) == 0, low, high)
        pick_2 = lax.shift_right_arithmetic(found, log2(nblk))
        slot_own_2[...] = found & (nblk - 1)
        row = rows_of((8, 128))
        idx_v[...] = jnp.where(
            row == PICK_1, pick_1, jnp.where(row == PICK_2, pick_2, idx_v[...])
        )
        slot_in_1[0] = slot_own_1[...]
        slot_in_2[0] = slot_own_2[...]

        def to_member(step, carry):
            pltpu.make_async_remote_copy(
                slot_own_1, slot_in_1.at[step], meta_send.at[2], meta_recv.at[2],
                at_member(step), MESH,
            ).start()
            return carry

        def to_group(step, carry):
            pltpu.make_async_remote_copy(
                slot_own_2, slot_in_2.at[step], meta_send.at[3], meta_recv.at[3],
                at_group(step), MESH,
            ).start()
            return carry

        lax.fori_loop(1, nd, to_member, 0)
        lax.fori_loop(1, ng, to_group, 0)
        publish()

    def final_tables():
        wait_bytes(meta_recv.at[2], slot_in_1.at[pl.ds(1, nd - 1)])
        wait_bytes(meta_recv.at[3], slot_in_2.at[pl.ds(1, ng - 1)])

        def place(table, lane_of_row, number):
            lane, row = lanes(table.shape), rows_of(table.shape)
            slot = jnp.sum(
                jnp.where(lane == lane_of_row(row), table, 0).astype(F32), axis=1, keepdims=True
            ).astype(jnp.int32)
            slot = jnp.where(column(row, 0) < number, slot, -7)
            hit = jnp.where(slot == lane, lane_of_row(row), 0)
            return jnp.broadcast_to(jnp.sum(hit, axis=0, keepdims=True), (8, 128))

        table = stack_rows(slot_in_1, nd)
        slot_1 = place(table, lambda row: row, nd)
        table = stack_rows(slot_in_2, ng)
        slot_2 = place(table, lambda row: 2 * row, ng) + place(table, lambda row: 2 * row + 1, ng)
        row = rows_of((8, 128))
        idx_v[...] = jnp.where(
            row == SLOT_1, slot_1, jnp.where(row == SLOT_2, slot_2, idx_v[...])
        )
        publish()

    def look(row, lane):
        return idx[row, lane] & (nblk - 1)

    def remote(src, dst, stage, c, where):
        return pltpu.make_async_remote_copy(
            src, dst, data_send.at[stage, c], data_recv.at[stage, c], where, MESH
        )

    def to_groups(src, dst, stage, c):
        def step(number, carry):
            span = pl.ds(2 * number, 2)
            remote(src.at[span], dst.at[span], stage, c, at_group(number)).start()
            return carry

        lax.fori_loop(1, ng, step, 0)

    def to_members(src, dst, stage, c):
        def step(number, carry):
            remote(src.at[number], dst.at[number], stage, c, at_member(number)).start()
            return carry

        lax.fori_loop(1, nd, step, 0)

    def far(ref, by_group):
        return ref.at[pl.ds(2, nblk - 2)] if by_group else ref.at[pl.ds(1, nd - 1)]

    def send_first(c):
        (to_groups if c % 2 else to_members)(send_a[c], recv_a[c], 0, c)

    def send_second(c):
        wait_bytes(data_recv.at[0, c], far(recv_a[c], c % 2))
        near = 1 if c % 2 else 2
        pick = PICK_1 if c % 2 else PICK_2
        for k in range(near):
            recv_b[c][k] = recv_a[c][look(pick, k)]

        def step(number, carry):
            for k in range(near):
                send_b[c][near * number + k] = recv_a[c][look(pick, near * number + k)]
            span = pl.ds(near * number, near)
            where = at_member(number) if c % 2 else at_group(number)
            remote(send_b[c].at[span], recv_b[c].at[span], 1, c, where).start()
            return carry

        lax.fori_loop(1, nblk // near, step, 0)

    def deliver(c):
        wait_bytes(data_recv.at[1, c], far(recv_b[c], c % 2 == 0))

        def step(number, carry):
            for s in (2 * number, 2 * number + 1):
                slot = look(SLOT_1 if c % 2 else SLOT_2, s)
                out_ref[s, c * piece : (c + 1) * piece, :] = recv_b[c][slot]
            return carry

        lax.fori_loop(0, nblk // 2, step, 0)

    def prepare_prefix():
        load_keys.wait()
        for first in range(0, prefix, KEY_TILE):
            span = slice(first, first + KEY_TILE)
            keys_t[:, span] = keys[span, :].T
        load_values.wait()
        load_length.wait()
        live = length_ref[0]
        for first in range(0, prefix, KEY_TILE):
            span = slice(first, first + KEY_TILE)
            shape = (KEY_TILE, width)
            values[span, :] = jnp.where(
                rows_of(shape) + first < live, values[span, :], jnp.zeros(shape, BF16)
            )

    score_scale = 0.5 / (head_dim**0.5)

    def order_of(t):
        return jnp.where(t % 2 == 1, ORDER_G, ORDER_D)

    def rows_in_order(ref, t, first_row):
        row = order_of(t)
        parts = [
            ref[look(row, place), pl.ds(first_row, piece), :] for place in range(nblk)
        ]
        return jnp.concatenate(parts, axis=0).astype(F32)

    def normalise_rows(ref, t, first_row):
        x = rows_in_order(ref, t, first_row)
        nrm[...] = (centre(x, width) * (gain_ref[...] * 0.5)).astype(BF16)

    def project(first):
        half = jnp.dot(nrm[...], win[:, first : first + COLS], preferred_element_type=F32)
        return half_silu(half + bias_ref[:, first : first + COLS] * 0.5)

    def project_qkv():
        for first in range(width, 4 * width, COLS):
            act = project(first)
            if 2 * width <= first < 3 * width:
                act = act * score_scale
            qkv[:, first - width : first - width + COLS] = act.astype(BF16)

    def attend(following):
        for first in range(0, width, COLS):
            gate[:, first : first + COLS] = project(first).astype(BF16)
        tiles = [(h, first) for h in range(HEADS) for first in range(0, prefix, KEY_TILE)]

        def part_of(group, h):
            first = group * width + h * head_dim
            return qkv[:, first : first + head_dim]

        def score(tile):
            h, first = tile
            cols = slice(h * head_dim, (h + 1) * head_dim)
            return jnp.dot(
                part_of(1, h), keys_t[cols, first : first + KEY_TILE], preferred_element_type=F32
            )

        ahead = [score(tile) for tile in tiles[:AHEAD]]
        totals = [None] * HEADS
        for number, (h, first) in enumerate(tiles):
            half = ahead.pop(0)
            if number + AHEAD < len(tiles):
                ahead.append(score(tiles[number + AHEAD]))
            cols = slice(h * head_dim, (h + 1) * head_dim)
            weights = half_silu(half).astype(BF16)
            term = jnp.dot(
                weights, values[first : first + KEY_TILE, cols], preferred_element_type=F32
            )
            totals[h] = term if totals[h] is None else totals[h] + term
            if first + KEY_TILE == prefix:
                own = jnp.sum(
                    part_of(1, h).astype(F32) * part_of(2, h).astype(F32), axis=-1, keepdims=True
                )
                own = half_silu(own).astype(BF16).astype(F32)
                att[:, cols] = totals[h] + own * part_of(0, h).astype(F32)
                if h == 0 and following is not None:
                    following()

    def finish_gate():
        return (
            centre(att[...], width) * again_ref[...] * gate[...].astype(F32)
        ).astype(BF16)

    def finish(t, gated):
        first_row = pl.multiple_of(t * piece, piece)
        delta = jnp.dot(gated, wout[...], preferred_element_type=F32)
        row = order_of(t)
        count = count_ref[0]
        done = []
        for place in range(nblk):
            block = look(row, place)
            x = cand[block, pl.ds(first_row, piece), :].astype(F32)
            x = x + delta[place * piece : (place + 1) * piece, :]
            live = rows_of((piece, width)) + (block * BLK + first_row) < count
            done.append(jnp.where(live, x, 0.0).astype(BF16))
        return done

    def exchange(t, done):
        for c in range(CHUNKS):

            @pl.when(t == c)
            def _():
                near = 2 if c % 2 else 1
                for place in range(nblk):
                    (recv_a[c] if place < near else send_a[c])[place] = done[place]
                send_first(c)
                if c == LAG:
                    middle_tables()
                if c >= LAG:
                    send_second(c - LAG)
                if c == LAST_LAG:
                    final_tables()
                if c >= LAST_LAG:
                    deliver(c - LAST_LAG)

    load_device.wait()
    load_slot.wait()
    own_table()
    publish()
    load_first.wait()
    load_gain.wait()
    normalise_rows(cand_first, 0, 0)
    load_bias.wait()
    load_win.wait()
    project_qkv()
    prepare_prefix()
    load_cand.wait()

    def next_rows(t):
        normalise_rows(cand, t, pl.multiple_of(t * piece, piece))

    attend(lambda: next_rows(1))
    load_again.wait()
    load_count.wait()
    load_wout.wait()
    pl.semaphore_wait(barrier, ng + nd - 2)
    send_tables()

    def step(t, carry):
        gated = finish_gate()
        project_qkv()
        done = finish(t - 1, gated)
        exchange(t - 1, done)
        attend(lambda: next_rows(jnp.minimum(t + 1, CHUNKS - 1)))
        return carry

    lax.fori_loop(1, CHUNKS, step, 0)
    last = CHUNKS - 1
    exchange(last, finish(last, finish_gate()))
    waiting = CHUNKS - LAST_LAG
    for c in range(CHUNKS - LAG, CHUNKS):
        send_second(c)
        if waiting < c - 1:
            deliver(waiting)
            waiting += 1
    for c in range(waiting, CHUNKS):
        deliver(c)

    wait_bytes(meta_send.at[0], tab_g.at[pl.ds(1, ng - 1)])
    wait_bytes(meta_send.at[1], tab_d.at[pl.ds(1, nd - 1)])
    wait_bytes(meta_send.at[2], slot_in_1.at[pl.ds(1, nd - 1)])
    wait_bytes(meta_send.at[3], slot_in_2.at[pl.ds(1, ng - 1)])
    for c in range(CHUNKS):
        wait_bytes(data_send.at[0, c], far(send_a[c], c % 2))
        wait_bytes(data_send.at[1, c], far(send_b[c], c % 2 == 0))


def layer(
    ng,
    nd,
    candidates,
    prefix_keys,
    prefix_values,
    cand_count,
    prefix_len,
    dest_device,
    dest_slot,
    norm_gain,
    w_in,
    b_in,
    attn_gain,
    w_out,
):
    rows, width = candidates.shape
    prefix = prefix_keys.shape[1]
    nblk = rows // BLK
    piece = BLK // CHUNKS
    tile_rows = nblk * piece
    hbm = pl.BlockSpec(memory_space=pl.ANY)
    block = pltpu.VMEM((nblk, piece, width), BF16)
    table = pltpu.VMEM((8, 128), jnp.int32)
    out = pl.pallas_call(
        functools.partial(kernel, (ng, nd, nblk, width, prefix)),
        out_shape=jax.ShapeDtypeStruct((nblk, BLK, width), BF16),
        in_specs=[hbm] * 12,
        out_specs=pl.BlockSpec(memory_space=pltpu.VMEM),
        scratch_shapes=[
            pltpu.SMEM((1,), jnp.int32),
            pltpu.SMEM((1,), jnp.int32),
            pltpu.VMEM((1, nblk), jnp.int32),
            pltpu.VMEM((1, nblk), jnp.int32),
            pltpu.VMEM((1, width), F32),
            pltpu.VMEM((1, 4 * width), F32),
            pltpu.VMEM((1, width), F32),
            block,
            pltpu.VMEM((nblk, BLK, width), BF16),
            pltpu.VMEM((prefix, width), BF16),
            pltpu.VMEM((width, prefix), BF16),
            pltpu.VMEM((prefix, width), BF16),
            pltpu.VMEM((width, 4 * width), BF16),
            pltpu.VMEM((width, width), BF16),
            pltpu.VMEM((tile_rows, width), BF16),
            pltpu.VMEM((tile_rows, width), BF16),
            pltpu.VMEM((tile_rows, 3 * width), BF16),
            pltpu.VMEM((tile_rows, width), F32),
            table,
            pltpu.VMEM((ng, 8, 128), jnp.int32),
            pltpu.VMEM((nd, 8, 128), jnp.int32),
            table,
            table,
            pltpu.VMEM((nd, 8, 128), jnp.int32),
            pltpu.VMEM((ng, 8, 128), jnp.int32),
            table,
            pltpu.SMEM((8, 128), jnp.int32),
            pltpu.SemaphoreType.DMA((13,)),
            pltpu.SemaphoreType.DMA,
            pltpu.SemaphoreType.DMA((4,)),
            pltpu.SemaphoreType.DMA((4,)),
            pltpu.SemaphoreType.DMA((2, CHUNKS)),
            pltpu.SemaphoreType.DMA((2, CHUNKS)),
        ]
        + [block] * (4 * CHUNKS),
        compiler_params=pltpu.CompilerParams(
            collective_id=0, has_side_effects=True, vmem_limit_bytes=60 * 2**20
        ),
    )(
        cand_count,
        prefix_len,
        dest_device.reshape(1, nblk),
        dest_slot.reshape(1, nblk),
        norm_gain.reshape(1, width),
        b_in.reshape(1, 4 * width),
        attn_gain.reshape(1, width),
        candidates.reshape(nblk, BLK, width),
        prefix_keys[0],
        prefix_values[0],
        w_in,
        w_out,
    )
    return out.reshape(rows, width)


def solution(mesh):
    spec = P(("grp", "dev"))
    wide = P(("grp", "dev"), None)
    deep = P(("grp", "dev"), None, None)
    return jax.shard_map(
        functools.partial(layer, mesh.shape["grp"], mesh.shape["dev"]),
        mesh=mesh,
        in_specs=(wide, deep, deep, spec, spec, spec, spec, P(), P(), P(), P(), P()),
        out_specs=wide,
        check_vma=False,
    )
```

```python
import functools

import jax
import jax.numpy as jnp
from jax import lax
from jax.experimental import pallas as pl
from jax.experimental.pallas import tpu as pltpu
from jax.sharding import PartitionSpec as P

HEADS = 4
BLK = 128
CHUNKS = 8
LAG = 4
LAST_LAG = 7
HALVED = (6, 7)
KEY_TILE = 256
AHEAD = 2
COLS = 256
MESH = pl.DeviceIdType.MESH
F32 = jnp.float32
BF16 = jnp.bfloat16
ORDER_G, ORDER_D, PICK_1, PICK_2, SLOT_1, SLOT_2, MOVE = range(7)


def in_hbm(array):
    return pltpu.with_memory_space_constraint(array, pltpu.HBM)


def log2(number):
    return number.bit_length() - 1


def lanes(shape):
    return lax.broadcasted_iota(jnp.int32, shape, 1)


def rows_of(shape):
    return lax.broadcasted_iota(jnp.int32, shape, 0)


def stack_rows(ref, count):
    tiles = []
    for first in range(0, count, 8):
        tile = jnp.full((8, 128), -1, jnp.int32)
        for step in range(first, min(first + 8, count)):
            tile = jnp.where(rows_of((8, 128)) == step - first, ref[step], tile)
        tiles.append(tile)
    return tiles[0] if len(tiles) == 1 else jnp.concatenate(tiles, axis=0)


def column(matrix, index):
    return matrix[:, index : index + 1]


def centre(matrix, width):
    average = jnp.sum(matrix, axis=-1, keepdims=True) * (1.0 / width)
    centred = matrix - average
    spread = jnp.sum(centred * centred, axis=-1, keepdims=True) * (1.0 / width)
    return centred * lax.rsqrt(spread + 1e-06)


def routes_of(width):
    routes = []
    for c in range(CHUNKS):
        if c in HALVED:
            routes += [(c, way, way * (width // 2), width // 2) for way in (0, 1)]
        else:
            routes.append((c, c % 2, 0, width))
    return routes


def half_silu(half):
    return half + half * jnp.tanh(half)


def kernel(sizes, *refs):
    ng, nd, nblk, width, prefix = sizes
    piece = BLK // CHUNKS
    tile_rows = nblk * piece
    head_dim = width // HEADS
    (
        count_hbm,
        length_hbm,
        device_hbm,
        slot_hbm,
        gain_hbm,
        bias_hbm,
        again_hbm,
        cand_hbm,
        key_hbm,
        value_hbm,
        win_hbm,
        wout_hbm,
        out_ref,
        count_ref,
        length_ref,
        device_ref,
        slot_ref,
        gain_ref,
        bias_ref,
        again_ref,
        cand_first,
        cand,
        keys,
        keys_t,
        values,
        win,
        wout,
        whole,
        nrm,
        gate,
        qkv,
        att,
        tab_own,
        tab_g,
        tab_d,
        slot_own_1,
        slot_own_2,
        slot_in_1,
        slot_in_2,
        idx_v,
        idx,
        load_sem,
        idx_sem,
        meta_send,
        meta_recv,
        data_send,
        data_recv,
        *bufs,
    ) = refs
    routes = routes_of(width)
    send_a, recv_a, send_b, recv_b = (
        bufs[len(routes) * k : len(routes) * (k + 1)] for k in range(4)
    )
    me_g = lax.axis_index("grp")
    me_d = lax.axis_index("dev")

    def at_group(step):
        return {"grp": (me_g + step) & (ng - 1), "dev": me_d}

    def at_member(step):
        return {"grp": me_g, "dev": (me_d + step) & (nd - 1)}

    (
        load_device,
        load_slot,
        load_gain,
        load_bias,
        load_again,
        load_count,
        load_length,
        load_first,
        load_win,
        load_keys,
        load_values,
        load_cand,
        load_wout,
    ) = loads = [
        pltpu.make_async_copy(src, dst, load_sem.at[k])
        for k, (src, dst) in enumerate(
            (
                (device_hbm, device_ref),
                (slot_hbm, slot_ref),
                (gain_hbm, gain_ref),
                (bias_hbm, bias_ref),
                (again_hbm, again_ref),
                (count_hbm, count_ref),
                (length_hbm, length_ref),
                (cand_hbm.at[:, pl.ds(0, piece), :], cand_first),
                (win_hbm, win),
                (key_hbm, keys),
                (value_hbm, values),
                (cand_hbm, cand),
                (wout_hbm, wout),
            )
        )
    ]
    for load in loads:
        load.start()

    barrier = pltpu.get_barrier_semaphore()

    def greet_group(step, carry):
        pl.semaphore_signal(barrier, inc=1, device_id=at_group(step), device_id_type=MESH)
        return carry

    def greet_member(step, carry):
        pl.semaphore_signal(barrier, inc=1, device_id=at_member(step), device_id_type=MESH)
        return carry

    lax.fori_loop(1, ng, greet_group, 0)
    lax.fori_loop(1, nd, greet_member, 0)

    def own_table():
        tab_own[...] = jnp.full((8, 128), -1, jnp.int32)
        code = device_ref[...] * nblk + slot_ref[...]
        tab_own[:, 0:nblk] = jnp.broadcast_to(code, (8, nblk))
        table = tab_own[...]
        device = lax.shift_right_arithmetic(table, log2(nblk))
        group = lax.shift_right_arithmetic(device, log2(nd))
        member = jnp.where(table < 0, -1, device & (nd - 1))
        lane = lanes((8, 128))
        live = lane < nblk
        want_g = jnp.where(
            live, (me_g + lax.shift_right_arithmetic(lane, 1)) & (ng - 1), -7
        )
        want_d = jnp.where(live, (me_d + lane) & (nd - 1), -7)
        low = jnp.full((8, 128), nblk - 1, jnp.int32)
        high = jnp.zeros((8, 128), jnp.int32)
        order_d = jnp.zeros((8, 128), jnp.int32)
        for i in range(nblk):
            hit_g = column(group, i) == want_g
            low = jnp.where(hit_g, jnp.minimum(low, i), low)
            high = jnp.where(hit_g, jnp.maximum(high, i), high)
            order_d = jnp.where(column(member, i) == want_d, i, order_d)
        order_g = jnp.where((lane & 1) == 0, low, high)
        move = jnp.zeros((8, 128), jnp.int32)
        for place in range(nblk):
            move = jnp.where(column(order_g, place) == order_d, place, move)
        row = rows_of((8, 128))
        idx_v[...] = jnp.where(
            row == ORDER_G,
            order_g,
            jnp.where(row == ORDER_D, order_d, jnp.where(row == MOVE, move, 0)),
        )
        tab_g[0] = table
        tab_d[0] = table

    def publish():
        copy = pltpu.make_async_copy(idx_v, idx, idx_sem)
        copy.start()
        copy.wait()

    def send_tables():
        def to_group(step, carry):
            pltpu.make_async_remote_copy(
                tab_own, tab_g.at[step], meta_send.at[0], meta_recv.at[0], at_group(step), MESH
            ).start()
            return carry

        def to_member(step, carry):
            pltpu.make_async_remote_copy(
                tab_own, tab_d.at[step], meta_send.at[1], meta_recv.at[1], at_member(step), MESH
            ).start()
            return carry

        lax.fori_loop(1, ng, to_group, 0)
        lax.fori_loop(1, nd, to_member, 0)

    def wait_bytes(sem, ref):
        pltpu.make_async_copy(ref, ref, sem).wait()

    def middle_tables():
        wait_bytes(meta_recv.at[0], tab_g.at[pl.ds(1, ng - 1)])
        wait_bytes(meta_recv.at[1], tab_d.at[pl.ds(1, nd - 1)])
        table = stack_rows(tab_g, ng)
        shape = table.shape
        device = lax.shift_right_arithmetic(table, log2(nblk))
        group = lax.shift_right_arithmetic(device, log2(nd))
        slot = table & (nblk - 1)
        lane = lanes(shape)
        mine = group == me_g
        first = jnp.min(
            jnp.where(mine, lane.astype(F32), 1000.0), axis=1, keepdims=True
        ).astype(jnp.int32)
        place = 2 * rows_of(shape) + jnp.where(lane > first, 1, 0)
        both = place * nblk + slot
        want = jnp.where(lane < nblk, me_g * nd + ((me_d + lane) & (nd - 1)), -7)
        found = jnp.zeros(shape, jnp.int32)
        for i in range(nblk):
            found = found + jnp.where(column(device, i) == want, column(both, i), 0)
        found = jnp.sum(found, axis=0, keepdims=True)
        found = jnp.broadcast_to(found, (8, 128))
        pick_1 = lax.shift_right_arithmetic(found, log2(nblk))
        slot_own_1[...] = found & (nblk - 1)
        table = stack_rows(tab_d, nd)
        shape = table.shape
        device = lax.shift_right_arithmetic(table, log2(nblk))
        both = rows_of(shape) * nblk + (table & (nblk - 1))
        lane = lanes(shape)
        want = jnp.where(
            lane < nblk,
            ((me_g + lax.shift_right_arithmetic(lane, 1)) & (ng - 1)) * nd + me_d,
            -7,
        )
        top = nd * nblk - 1
        low = jnp.full(shape, top, jnp.int32)
        high = jnp.zeros(shape, jnp.int32)
        for i in range(nblk):
            hit = column(device, i) == want
            low = jnp.where(hit, jnp.minimum(low, column(both, i)), low)
            high = jnp.where(hit, jnp.maximum(high, column(both, i)), high)
        low = jnp.broadcast_to(jnp.min(low, axis=0, keepdims=True), (8, 128))
        high = jnp.broadcast_to(jnp.max(high, axis=0, keepdims=True), (8, 128))
        found = jnp.where((lanes((8, 128)) & 1) == 0, low, high)
        pick_2 = lax.shift_right_arithmetic(found, log2(nblk))
        slot_own_2[...] = found & (nblk - 1)
        row = rows_of((8, 128))
        idx_v[...] = jnp.where(
            row == PICK_1, pick_1, jnp.where(row == PICK_2, pick_2, idx_v[...])
        )
        slot_in_1[0] = slot_own_1[...]
        slot_in_2[0] = slot_own_2[...]

        def to_member(step, carry):
            pltpu.make_async_remote_copy(
                slot_own_1, slot_in_1.at[step], meta_send.at[2], meta_recv.at[2],
                at_member(step), MESH,
            ).start()
            return carry

        def to_group(step, carry):
            pltpu.make_async_remote_copy(
                slot_own_2, slot_in_2.at[step], meta_send.at[3], meta_recv.at[3],
                at_group(step), MESH,
            ).start()
            return carry

        lax.fori_loop(1, nd, to_member, 0)
        lax.fori_loop(1, ng, to_group, 0)
        publish()

    def final_tables():
        wait_bytes(meta_recv.at[2], slot_in_1.at[pl.ds(1, nd - 1)])
        wait_bytes(meta_recv.at[3], slot_in_2.at[pl.ds(1, ng - 1)])

        def place(table, lane_of_row, number):
            lane, row = lanes(table.shape), rows_of(table.shape)
            slot = jnp.sum(
                jnp.where(lane == lane_of_row(row), table, 0).astype(F32), axis=1, keepdims=True
            ).astype(jnp.int32)
            slot = jnp.where(column(row, 0) < number, slot, -7)
            hit = jnp.where(slot == lane, lane_of_row(row), 0)
            return jnp.broadcast_to(jnp.sum(hit, axis=0, keepdims=True), (8, 128))

        table = stack_rows(slot_in_1, nd)
        slot_1 = place(table, lambda row: row, nd)
        table = stack_rows(slot_in_2, ng)
        slot_2 = place(table, lambda row: 2 * row, ng) + place(table, lambda row: 2 * row + 1, ng)
        row = rows_of((8, 128))
        idx_v[...] = jnp.where(
            row == SLOT_1, slot_1, jnp.where(row == SLOT_2, slot_2, idx_v[...])
        )
        publish()

    def look(row, lane):
        return idx[row, lane] & (nblk - 1)

    def remote(src, dst, stage, r, where):
        return pltpu.make_async_remote_copy(
            src, dst, data_send.at[stage, r], data_recv.at[stage, r], where, MESH
        )

    def to_groups(src, dst, stage, r):
        def step(number, carry):
            span = pl.ds(2 * number, 2)
            remote(src.at[span], dst.at[span], stage, r, at_group(number)).start()
            return carry

        lax.fori_loop(1, ng, step, 0)

    def to_members(src, dst, stage, r):
        def step(number, carry):
            remote(src.at[number], dst.at[number], stage, r, at_member(number)).start()
            return carry

        lax.fori_loop(1, nd, step, 0)

    def far(ref, by_group):
        return ref.at[pl.ds(2, nblk - 2)] if by_group else ref.at[pl.ds(1, nd - 1)]

    def send_first(r):
        way = routes[r][1]
        (to_groups if way else to_members)(send_a[r], recv_a[r], 0, r)

    def send_second(r):
        way = routes[r][1]
        wait_bytes(data_recv.at[0, r], far(recv_a[r], way))
        near = 1 if way else 2
        pick = PICK_1 if way else PICK_2
        for k in range(near):
            recv_b[r][k] = recv_a[r][look(pick, k)]

        def step(number, carry):
            for k in range(near):
                send_b[r][near * number + k] = recv_a[r][look(pick, near * number + k)]
            span = pl.ds(near * number, near)
            where = at_member(number) if way else at_group(number)
            remote(send_b[r].at[span], recv_b[r].at[span], 1, r, where).start()
            return carry

        lax.fori_loop(1, nblk // near, step, 0)

    def deliver(r):
        c, way, first, wide = routes[r]
        wait_bytes(data_recv.at[1, r], far(recv_b[r], not way))

        def step(number, carry):
            for s in (2 * number, 2 * number + 1):
                slot = look(SLOT_1 if way else SLOT_2, s)
                out_ref[s, c * piece : (c + 1) * piece, first : first + wide] = recv_b[r][slot]
            return carry

        lax.fori_loop(0, nblk // 2, step, 0)

    def each_route(action, c):
        for r, route in enumerate(routes):
            if route[0] == c:
                action(r)

    def prepare_prefix():
        load_keys.wait()
        for first in range(0, prefix, KEY_TILE):
            span = slice(first, first + KEY_TILE)
            keys_t[:, span] = keys[span, :].T
        load_values.wait()
        load_length.wait()
        live = length_ref[0]
        for first in range(0, prefix, KEY_TILE):
            span = slice(first, first + KEY_TILE)
            shape = (KEY_TILE, width)
            values[span, :] = jnp.where(
                rows_of(shape) + first < live, values[span, :], jnp.zeros(shape, BF16)
            )

    score_scale = 0.5 / (head_dim**0.5)

    def order_of(t):
        by_group = t % 2 == 1
        for c in HALVED:
            by_group = jnp.logical_or(by_group, t == c)
        return jnp.where(by_group, ORDER_G, ORDER_D)

    def rows_in_order(ref, t, first_row):
        row = order_of(t)
        parts = [
            ref[look(row, place), pl.ds(first_row, piece), :] for place in range(nblk)
        ]
        return jnp.concatenate(parts, axis=0).astype(F32)

    def normalise_rows(ref, t, first_row):
        if ref is cand_first:
            x = cand_first[...].reshape(tile_rows, width).astype(F32)
        else:
            x = rows_in_order(ref, t, first_row)
        nrm[...] = (centre(x, width) * (gain_ref[...] * 0.5)).astype(BF16)

    def project(first):
        half = jnp.dot(nrm[...], win[:, first : first + COLS], preferred_element_type=F32)
        return half_silu(half + bias_ref[:, first : first + COLS] * 0.5)

    def project_qkv():
        for first in range(width, 4 * width, COLS):
            act = project(first)
            if 2 * width <= first < 3 * width:
                act = act * score_scale
            qkv[:, first - width : first - width + COLS] = act.astype(BF16)

    def attend(following):
        for first in range(0, width, COLS):
            gate[:, first : first + COLS] = project(first).astype(BF16)
        tiles = [(h, first) for h in range(HEADS) for first in range(0, prefix, KEY_TILE)]

        def part_of(group, h):
            first = group * width + h * head_dim
            return qkv[:, first : first + head_dim]

        def score(tile):
            h, first = tile
            cols = slice(h * head_dim, (h + 1) * head_dim)
            return jnp.dot(
                part_of(1, h), keys_t[cols, first : first + KEY_TILE], preferred_element_type=F32
            )

        ahead = [score(tile) for tile in tiles[:AHEAD]]
        totals = [None] * HEADS
        for number, (h, first) in enumerate(tiles):
            half = ahead.pop(0)
            if number + AHEAD < len(tiles):
                ahead.append(score(tiles[number + AHEAD]))
            cols = slice(h * head_dim, (h + 1) * head_dim)
            weights = half_silu(half).astype(BF16)
            term = jnp.dot(
                weights, values[first : first + KEY_TILE, cols], preferred_element_type=F32
            )
            totals[h] = term if totals[h] is None else totals[h] + term
            if first + KEY_TILE == prefix:
                own = jnp.sum(
                    part_of(1, h).astype(F32) * part_of(2, h).astype(F32), axis=-1, keepdims=True
                )
                own = half_silu(own).astype(BF16).astype(F32)
                att[:, cols] = totals[h] + own * part_of(0, h).astype(F32)
                if h == 0 and following is not None:
                    following()

    def finish_gate():
        return (
            centre(att[...], width) * again_ref[...] * gate[...].astype(F32)
        ).astype(BF16)

    def finish(t, gated, stored_order=False):
        first_row = t * piece if stored_order else pl.multiple_of(t * piece, piece)
        delta = jnp.dot(gated, wout[...], preferred_element_type=F32)
        row = order_of(t)
        count = count_ref[0]
        done = []
        for place in range(nblk):
            block = place if stored_order else look(row, place)
            x = cand[block, pl.ds(first_row, piece), :].astype(F32)
            x = x + delta[place * piece : (place + 1) * piece, :]
            live = rows_of((piece, width)) + (block * BLK + first_row) < count
            done.append(jnp.where(live, x, 0.0).astype(BF16))
        return done

    def store(c, done):
        if c in HALVED:
            for place in range(nblk):
                whole[place] = done[place]

        def keep(r):
            way, first, wide = routes[r][1:]
            near = 2 if way else 1
            for place in range(nblk):
                target = recv_a[r] if place < near else send_a[r]
                if c in HALVED and not way:
                    target[place] = whole[look(MOVE, place), :, first : first + wide]
                else:
                    target[place] = done[place][:, first : first + wide]
            send_first(r)

        each_route(keep, c)

    def serve(c):
        if c == LAG:
            middle_tables()
        if 0 <= c - LAG < CHUNKS:
            each_route(send_second, c - LAG)
        if c == LAST_LAG:
            final_tables()
        if 0 <= c - LAST_LAG < CHUNKS:
            each_route(deliver, c - LAST_LAG)

    def exchange(t, done):
        for c in range(1, CHUNKS):

            @pl.when(t == c)
            def _():
                store(c, done)
                serve(c)

    load_first.wait()
    load_gain.wait()
    normalise_rows(cand_first, 0, 0)
    load_device.wait()
    load_slot.wait()
    own_table()
    load_bias.wait()
    load_win.wait()
    project_qkv()
    prepare_prefix()
    publish()
    load_cand.wait()

    def next_rows(t):
        normalise_rows(cand, t, pl.multiple_of(t * piece, piece))

    attend(lambda: next_rows(1))
    load_again.wait()
    load_count.wait()
    load_wout.wait()
    done = finish(0, finish_gate(), True)
    for place in range(nblk):
        whole[place] = done[place]
    done = [whole[look(ORDER_D, place)] for place in range(nblk)]
    pl.semaphore_wait(barrier, ng + nd - 2)
    store(0, done)
    send_tables()
    project_qkv()
    attend(lambda: next_rows(2))

    def step(t, carry):
        gated = finish_gate()
        project_qkv()
        done = finish(t - 1, gated)
        exchange(t - 1, done)
        attend(lambda: next_rows(jnp.minimum(t + 1, CHUNKS - 1)))
        return carry

    lax.fori_loop(2, CHUNKS, step, 0)
    last = CHUNKS - 1
    store(last, finish(last, finish_gate()))
    serve(last)
    waiting = CHUNKS - LAST_LAG
    for c in range(CHUNKS - LAG, CHUNKS):
        each_route(send_second, c)
        if waiting < c - 1:
            each_route(deliver, waiting)
            waiting += 1
    for c in range(waiting, CHUNKS):
        each_route(deliver, c)

    wait_bytes(meta_send.at[0], tab_g.at[pl.ds(1, ng - 1)])
    wait_bytes(meta_send.at[1], tab_d.at[pl.ds(1, nd - 1)])
    wait_bytes(meta_send.at[2], slot_in_1.at[pl.ds(1, nd - 1)])
    wait_bytes(meta_send.at[3], slot_in_2.at[pl.ds(1, ng - 1)])
    for r, route in enumerate(routes):
        wait_bytes(data_send.at[0, r], far(send_a[r], route[1]))
        wait_bytes(data_send.at[1, r], far(send_b[r], not route[1]))


def layer(
    ng,
    nd,
    candidates,
    prefix_keys,
    prefix_values,
    cand_count,
    prefix_len,
    dest_device,
    dest_slot,
    norm_gain,
    w_in,
    b_in,
    attn_gain,
    w_out,
):
    rows, width = candidates.shape
    prefix = prefix_keys.shape[1]
    nblk = rows // BLK
    piece = BLK // CHUNKS
    tile_rows = nblk * piece
    hbm = pl.BlockSpec(memory_space=pl.ANY)
    routes = routes_of(width)
    block = pltpu.VMEM((nblk, piece, width), BF16)
    table = pltpu.VMEM((8, 128), jnp.int32)
    out = pl.pallas_call(
        functools.partial(kernel, (ng, nd, nblk, width, prefix)),
        out_shape=jax.ShapeDtypeStruct((nblk, BLK, width), BF16),
        in_specs=[hbm] * 12,
        out_specs=pl.BlockSpec(memory_space=pltpu.VMEM),
        scratch_shapes=[
            pltpu.SMEM((1,), jnp.int32),
            pltpu.SMEM((1,), jnp.int32),
            pltpu.VMEM((1, nblk), jnp.int32),
            pltpu.VMEM((1, nblk), jnp.int32),
            pltpu.VMEM((1, width), F32),
            pltpu.VMEM((1, 4 * width), F32),
            pltpu.VMEM((1, width), F32),
            block,
            pltpu.VMEM((nblk, BLK, width), BF16),
            pltpu.VMEM((prefix, width), BF16),
            pltpu.VMEM((width, prefix), BF16),
            pltpu.VMEM((prefix, width), BF16),
            pltpu.VMEM((width, 4 * width), BF16),
            pltpu.VMEM((width, width), BF16),
            block,
            pltpu.VMEM((tile_rows, width), BF16),
            pltpu.VMEM((tile_rows, width), BF16),
            pltpu.VMEM((tile_rows, 3 * width), BF16),
            pltpu.VMEM((tile_rows, width), F32),
            table,
            pltpu.VMEM((ng, 8, 128), jnp.int32),
            pltpu.VMEM((nd, 8, 128), jnp.int32),
            table,
            table,
            pltpu.VMEM((nd, 8, 128), jnp.int32),
            pltpu.VMEM((ng, 8, 128), jnp.int32),
            table,
            pltpu.SMEM((8, 128), jnp.int32),
            pltpu.SemaphoreType.DMA((13,)),
            pltpu.SemaphoreType.DMA,
            pltpu.SemaphoreType.DMA((4,)),
            pltpu.SemaphoreType.DMA((4,)),
            pltpu.SemaphoreType.DMA((2, len(routes))),
            pltpu.SemaphoreType.DMA((2, len(routes))),
        ]
        + [pltpu.VMEM((nblk, piece, route[3]), BF16) for route in routes] * 4,
        compiler_params=pltpu.CompilerParams(
            collective_id=0, has_side_effects=True, vmem_limit_bytes=40 * 2**20
        ),
    )(
        cand_count,
        prefix_len,
        *map(
            in_hbm,
            (
                dest_device.reshape(1, nblk),
                dest_slot.reshape(1, nblk),
                norm_gain.reshape(1, width),
                b_in.reshape(1, 4 * width),
                attn_gain.reshape(1, width),
                candidates.reshape(nblk, BLK, width),
                prefix_keys[0],
                prefix_values[0],
                w_in,
                w_out,
            ),
        )
    )
    return out.reshape(rows, width)


def solution(mesh):
    spec = P(("grp", "dev"))
    wide = P(("grp", "dev"), None)
    deep = P(("grp", "dev"), None, None)
    return jax.shard_map(
        functools.partial(layer, mesh.shape["grp"], mesh.shape["dev"]),
        mesh=mesh,
        in_specs=(wide, deep, deep, spec, spec, spec, spec, P(), P(), P(), P(), P()),
        out_specs=wide,
        check_vma=False,
    )
```

```python
import functools

import jax
import jax.numpy as jnp
from jax import lax
from jax.experimental import pallas as pl
from jax.experimental.pallas import tpu as pltpu
from jax.sharding import PartitionSpec as P

HEADS = 4
BLK = 128
CHUNKS = 8
LAG = 4
LAST_LAG = 8
HALVED = (1, 2, 3, 4, 5, 6, 7)
KEY_TILE = 256
AHEAD = 2
COLS = 256
MESH = pl.DeviceIdType.MESH
F32 = jnp.float32
BF16 = jnp.bfloat16
ORDER_G, ORDER_D, PICK_1, PICK_2, SLOT_1, SLOT_2, MOVE = range(7)


def in_hbm(array):
    return pltpu.with_memory_space_constraint(array, pltpu.HBM)


def log2(number):
    return number.bit_length() - 1


def lanes(shape):
    return lax.broadcasted_iota(jnp.int32, shape, 1)


def rows_of(shape):
    return lax.broadcasted_iota(jnp.int32, shape, 0)


def stack_rows(ref, count):
    tiles = []
    for first in range(0, count, 8):
        tile = jnp.full((8, 128), -1, jnp.int32)
        for step in range(first, min(first + 8, count)):
            tile = jnp.where(rows_of((8, 128)) == step - first, ref[step], tile)
        tiles.append(tile)
    return tiles[0] if len(tiles) == 1 else jnp.concatenate(tiles, axis=0)


def column(matrix, index):
    return matrix[:, index : index + 1]


def centre(matrix, width):
    average = jnp.sum(matrix, axis=-1, keepdims=True) * (1.0 / width)
    centred = matrix - average
    spread = jnp.sum(centred * centred, axis=-1, keepdims=True) * (1.0 / width)
    return centred * lax.rsqrt(spread + 1e-06)


def routes_of(width):
    routes = []
    for c in range(CHUNKS):
        if c in HALVED:
            routes += [(c, way, way * (width // 2), width // 2) for way in (0, 1)]
        else:
            routes.append((c, c % 2, 0, width))
    return routes


def half_silu(half):
    return half + half * jnp.tanh(half)


def kernel(sizes, *refs):
    ng, nd, nblk, width, prefix = sizes
    piece = BLK // CHUNKS
    tile_rows = nblk * piece
    head_dim = width // HEADS
    (
        count_hbm,
        length_hbm,
        device_hbm,
        slot_hbm,
        gain_hbm,
        bias_hbm,
        again_hbm,
        cand_hbm,
        key_hbm,
        value_hbm,
        win_hbm,
        wout_hbm,
        out_ref,
        count_ref,
        length_ref,
        device_ref,
        slot_ref,
        gain_ref,
        bias_ref,
        again_ref,
        cand_first,
        cand,
        keys,
        keys_t,
        values,
        win,
        wout,
        whole,
        nrm,
        gate,
        qkv,
        att,
        tab_own,
        tab_g,
        tab_d,
        slot_own_1,
        slot_own_2,
        slot_in_1,
        slot_in_2,
        idx_v,
        idx,
        load_sem,
        idx_sem,
        meta_send,
        meta_recv,
        data_send,
        data_recv,
        *bufs,
    ) = refs
    routes = routes_of(width)
    send_a, recv_a, send_b, recv_b = (
        bufs[len(routes) * k : len(routes) * (k + 1)] for k in range(4)
    )
    me_g = lax.axis_index("grp")
    me_d = lax.axis_index("dev")

    def at_group(step):
        return {"grp": (me_g + step) & (ng - 1), "dev": me_d}

    def at_member(step):
        return {"grp": me_g, "dev": (me_d + step) & (nd - 1)}

    (
        load_device,
        load_slot,
        load_gain,
        load_bias,
        load_again,
        load_count,
        load_length,
        load_first,
        load_win,
        load_keys,
        load_values,
        load_cand,
        load_wout,
    ) = loads = [
        pltpu.make_async_copy(src, dst, load_sem.at[k])
        for k, (src, dst) in enumerate(
            (
                (device_hbm, device_ref),
                (slot_hbm, slot_ref),
                (gain_hbm, gain_ref),
                (bias_hbm, bias_ref),
                (again_hbm, again_ref),
                (count_hbm, count_ref),
                (length_hbm, length_ref),
                (cand_hbm.at[:, pl.ds(0, piece), :], cand_first),
                (win_hbm, win),
                (key_hbm, keys),
                (value_hbm, values),
                (cand_hbm, cand),
                (wout_hbm, wout),
            )
        )
    ]
    for load in loads:
        load.start()

    barrier = pltpu.get_barrier_semaphore()

    def greet_group(step, carry):
        pl.semaphore_signal(barrier, inc=1, device_id=at_group(step), device_id_type=MESH)
        return carry

    def greet_member(step, carry):
        pl.semaphore_signal(barrier, inc=1, device_id=at_member(step), device_id_type=MESH)
        return carry

    lax.fori_loop(1, ng, greet_group, 0)
    lax.fori_loop(1, nd, greet_member, 0)

    def own_table():
        tab_own[...] = jnp.full((8, 128), -1, jnp.int32)
        code = device_ref[...] * nblk + slot_ref[...]
        tab_own[:, 0:nblk] = jnp.broadcast_to(code, (8, nblk))
        table = tab_own[...]
        device = lax.shift_right_arithmetic(table, log2(nblk))
        group = lax.shift_right_arithmetic(device, log2(nd))
        member = jnp.where(table < 0, -1, device & (nd - 1))
        lane = lanes((8, 128))
        live = lane < nblk
        want_g = jnp.where(
            live, (me_g + lax.shift_right_arithmetic(lane, 1)) & (ng - 1), -7
        )
        want_d = jnp.where(live, (me_d + lane) & (nd - 1), -7)
        low = jnp.full((8, 128), nblk - 1, jnp.int32)
        high = jnp.zeros((8, 128), jnp.int32)
        order_d = jnp.zeros((8, 128), jnp.int32)
        for i in range(nblk):
            hit_g = column(group, i) == want_g
            low = jnp.where(hit_g, jnp.minimum(low, i), low)
            high = jnp.where(hit_g, jnp.maximum(high, i), high)
            order_d = jnp.where(column(member, i) == want_d, i, order_d)
        order_g = jnp.where((lane & 1) == 0, low, high)
        move = jnp.zeros((8, 128), jnp.int32)
        for place in range(nblk):
            move = jnp.where(column(order_g, place) == order_d, place, move)
        row = rows_of((8, 128))
        idx_v[...] = jnp.where(
            row == ORDER_G,
            order_g,
            jnp.where(row == ORDER_D, order_d, jnp.where(row == MOVE, move, 0)),
        )
        tab_g[0] = table
        tab_d[0] = table

    def publish():
        copy = pltpu.make_async_copy(idx_v, idx, idx_sem)
        copy.start()
        copy.wait()

    def send_tables():
        def to_group(step, carry):
            pltpu.make_async_remote_copy(
                tab_own, tab_g.at[step], meta_send.at[0], meta_recv.at[0], at_group(step), MESH
            ).start()
            return carry

        def to_member(step, carry):
            pltpu.make_async_remote_copy(
                tab_own, tab_d.at[step], meta_send.at[1], meta_recv.at[1], at_member(step), MESH
            ).start()
            return carry

        lax.fori_loop(1, ng, to_group, 0)
        lax.fori_loop(1, nd, to_member, 0)

    def wait_bytes(sem, ref):
        pltpu.make_async_copy(ref, ref, sem).wait()

    def middle_tables():
        wait_bytes(meta_recv.at[0], tab_g.at[pl.ds(1, ng - 1)])
        wait_bytes(meta_recv.at[1], tab_d.at[pl.ds(1, nd - 1)])
        table = stack_rows(tab_g, ng)
        shape = table.shape
        device = lax.shift_right_arithmetic(table, log2(nblk))
        group = lax.shift_right_arithmetic(device, log2(nd))
        slot = table & (nblk - 1)
        lane = lanes(shape)
        mine = group == me_g
        first = jnp.min(
            jnp.where(mine, lane.astype(F32), 1000.0), axis=1, keepdims=True
        ).astype(jnp.int32)
        place = 2 * rows_of(shape) + jnp.where(lane > first, 1, 0)
        both = place * nblk + slot
        want = jnp.where(lane < nblk, me_g * nd + ((me_d + lane) & (nd - 1)), -7)
        found = jnp.zeros(shape, jnp.int32)
        for i in range(nblk):
            found = found + jnp.where(column(device, i) == want, column(both, i), 0)
        found = jnp.sum(found, axis=0, keepdims=True)
        found = jnp.broadcast_to(found, (8, 128))
        pick_1 = lax.shift_right_arithmetic(found, log2(nblk))
        slot_own_1[...] = found & (nblk - 1)
        table = stack_rows(tab_d, nd)
        shape = table.shape
        device = lax.shift_right_arithmetic(table, log2(nblk))
        both = rows_of(shape) * nblk + (table & (nblk - 1))
        lane = lanes(shape)
        want = jnp.where(
            lane < nblk,
            ((me_g + lax.shift_right_arithmetic(lane, 1)) & (ng - 1)) * nd + me_d,
            -7,
        )
        top = nd * nblk - 1
        low = jnp.full(shape, top, jnp.int32)
        high = jnp.zeros(shape, jnp.int32)
        for i in range(nblk):
            hit = column(device, i) == want
            low = jnp.where(hit, jnp.minimum(low, column(both, i)), low)
            high = jnp.where(hit, jnp.maximum(high, column(both, i)), high)
        low = jnp.broadcast_to(jnp.min(low, axis=0, keepdims=True), (8, 128))
        high = jnp.broadcast_to(jnp.max(high, axis=0, keepdims=True), (8, 128))
        found = jnp.where((lanes((8, 128)) & 1) == 0, low, high)
        pick_2 = lax.shift_right_arithmetic(found, log2(nblk))
        slot_own_2[...] = found & (nblk - 1)
        row = rows_of((8, 128))
        idx_v[...] = jnp.where(
            row == PICK_1, pick_1, jnp.where(row == PICK_2, pick_2, idx_v[...])
        )
        slot_in_1[0] = slot_own_1[...]
        slot_in_2[0] = slot_own_2[...]

        def to_member(step, carry):
            pltpu.make_async_remote_copy(
                slot_own_1, slot_in_1.at[step], meta_send.at[2], meta_recv.at[2],
                at_member(step), MESH,
            ).start()
            return carry

        def to_group(step, carry):
            pltpu.make_async_remote_copy(
                slot_own_2, slot_in_2.at[step], meta_send.at[3], meta_recv.at[3],
                at_group(step), MESH,
            ).start()
            return carry

        lax.fori_loop(1, nd, to_member, 0)
        lax.fori_loop(1, ng, to_group, 0)
        publish()

    def final_tables():
        wait_bytes(meta_recv.at[2], slot_in_1.at[pl.ds(1, nd - 1)])
        wait_bytes(meta_recv.at[3], slot_in_2.at[pl.ds(1, ng - 1)])

        def place(table, lane_of_row, number):
            lane, row = lanes(table.shape), rows_of(table.shape)
            slot = jnp.sum(
                jnp.where(lane == lane_of_row(row), table, 0).astype(F32), axis=1, keepdims=True
            ).astype(jnp.int32)
            slot = jnp.where(column(row, 0) < number, slot, -7)
            hit = jnp.where(slot == lane, lane_of_row(row), 0)
            return jnp.broadcast_to(jnp.sum(hit, axis=0, keepdims=True), (8, 128))

        table = stack_rows(slot_in_1, nd)
        slot_1 = place(table, lambda row: row, nd)
        table = stack_rows(slot_in_2, ng)
        slot_2 = place(table, lambda row: 2 * row, ng) + place(table, lambda row: 2 * row + 1, ng)
        row = rows_of((8, 128))
        idx_v[...] = jnp.where(
            row == SLOT_1, slot_1, jnp.where(row == SLOT_2, slot_2, idx_v[...])
        )
        publish()

    def look(row, lane):
        return idx[row, lane] & (nblk - 1)

    def remote(src, dst, stage, r, where):
        return pltpu.make_async_remote_copy(
            src, dst, data_send.at[stage, r], data_recv.at[stage, r], where, MESH
        )

    def to_groups(src, dst, stage, r):
        def step(number, carry):
            span = pl.ds(2 * number, 2)
            remote(src.at[span], dst.at[span], stage, r, at_group(number)).start()
            return carry

        lax.fori_loop(1, ng, step, 0, unroll=True)

    def to_members(src, dst, stage, r):
        def step(number, carry):
            remote(src.at[number], dst.at[number], stage, r, at_member(number)).start()
            return carry

        lax.fori_loop(1, nd, step, 0, unroll=True)

    def far(ref, by_group):
        return ref.at[pl.ds(2, nblk - 2)] if by_group else ref.at[pl.ds(1, nd - 1)]

    def send_first(r):
        way = routes[r][1]
        (to_groups if way else to_members)(send_a[r], recv_a[r], 0, r)

    def send_second(r):
        way = routes[r][1]
        wait_bytes(data_recv.at[0, r], far(recv_a[r], way))
        near = 1 if way else 2
        pick = PICK_1 if way else PICK_2
        for place in range(nblk):
            target = recv_b[r] if place < near else send_b[r]
            target[place] = recv_a[r][look(pick, place)]

        def step(number, carry):
            span = pl.ds(near * number, near)
            where = at_member(number) if way else at_group(number)
            remote(send_b[r].at[span], recv_b[r].at[span], 1, r, where).start()
            return carry

        lax.fori_loop(1, nblk // near, step, 0, unroll=True)

    def deliver(r):
        c, way, first, wide = routes[r]
        wait_bytes(data_recv.at[1, r], far(recv_b[r], not way))

        for s in range(nblk):
            slot = look(SLOT_1 if way else SLOT_2, s)
            out_ref[s, c * piece : (c + 1) * piece, first : first + wide] = recv_b[r][slot]

    def each_route(action, c):
        for r, route in enumerate(routes):
            if route[0] == c:
                action(r)

    def prepare_prefix():
        load_keys.wait()
        for first in range(0, prefix, KEY_TILE):
            span = slice(first, first + KEY_TILE)
            keys_t[:, span] = keys[span, :].T
        load_values.wait()
        load_length.wait()
        live = length_ref[0]
        for first in range(0, prefix, KEY_TILE):
            span = slice(first, first + KEY_TILE)
            shape = (KEY_TILE, width)
            values[span, :] = jnp.where(
                rows_of(shape) + first < live, values[span, :], jnp.zeros(shape, BF16)
            )

    score_scale = 0.5 / (head_dim**0.5)

    def order_of(t):
        by_group = t % 2 == 1
        for c in HALVED:
            by_group = jnp.logical_or(by_group, t == c)
        return jnp.where(by_group, ORDER_G, ORDER_D)

    def rows_in_order(ref, t, first_row):
        row = order_of(t)
        parts = [
            ref[look(row, place), pl.ds(first_row, piece), :] for place in range(nblk)
        ]
        return jnp.concatenate(parts, axis=0).astype(F32)

    def normalise_rows(ref, t, first_row):
        if ref is cand_first:
            x = cand_first[...].reshape(tile_rows, width).astype(F32)
        else:
            x = rows_in_order(ref, t, first_row)
        nrm[...] = (centre(x, width) * (gain_ref[...] * 0.5)).astype(BF16)

    def project(first):
        half = jnp.dot(nrm[...], win[:, first : first + COLS], preferred_element_type=F32)
        return half_silu(half + bias_ref[:, first : first + COLS] * 0.5)

    def project_qkv():
        for first in range(width, 4 * width, COLS):
            act = project(first)
            if 2 * width <= first < 3 * width:
                act = act * score_scale
            qkv[:, first - width : first - width + COLS] = act.astype(BF16)

    def attend(following):
        for first in range(0, width, COLS):
            gate[:, first : first + COLS] = project(first).astype(BF16)
        tiles = [(h, first) for h in range(HEADS) for first in range(0, prefix, KEY_TILE)]

        def part_of(group, h):
            first = group * width + h * head_dim
            return qkv[:, first : first + head_dim]

        def score(tile):
            h, first = tile
            cols = slice(h * head_dim, (h + 1) * head_dim)
            return jnp.dot(
                part_of(1, h), keys_t[cols, first : first + KEY_TILE], preferred_element_type=F32
            )

        ahead = [score(tile) for tile in tiles[:AHEAD]]
        totals = [None] * HEADS
        for number, (h, first) in enumerate(tiles):
            half = ahead.pop(0)
            if number + AHEAD < len(tiles):
                ahead.append(score(tiles[number + AHEAD]))
            cols = slice(h * head_dim, (h + 1) * head_dim)
            weights = half_silu(half).astype(BF16)
            term = jnp.dot(
                weights, values[first : first + KEY_TILE, cols], preferred_element_type=F32
            )
            totals[h] = term if totals[h] is None else totals[h] + term
            if first + KEY_TILE == prefix:
                own = jnp.sum(
                    part_of(1, h).astype(F32) * part_of(2, h).astype(F32), axis=-1, keepdims=True
                )
                own = half_silu(own).astype(BF16).astype(F32)
                att[:, cols] = totals[h] + own * part_of(0, h).astype(F32)
                if h == 0 and following is not None:
                    following()

    def finish_gate():
        return (
            centre(att[...], width) * again_ref[...] * gate[...].astype(F32)
        ).astype(BF16)

    def finish(t, gated, stored_order=False):
        first_row = t * piece if stored_order else pl.multiple_of(t * piece, piece)
        delta = jnp.dot(gated, wout[...], preferred_element_type=F32)
        row = order_of(t)
        count = count_ref[0]
        done = []
        for place in range(nblk):
            block = place if stored_order else look(row, place)
            x = cand[block, pl.ds(first_row, piece), :].astype(F32)
            x = x + delta[place * piece : (place + 1) * piece, :]
            live = rows_of((piece, width)) + (block * BLK + first_row) < count
            done.append(jnp.where(live, x, 0.0).astype(BF16))
        return done

    def store(c, done):
        if c in HALVED:
            for place in range(nblk):
                whole[place] = done[place]

        def keep(r):
            way, first, wide = routes[r][1:]
            near = 2 if way else 1
            for place in range(nblk):
                target = recv_a[r] if place < near else send_a[r]
                if c in HALVED and not way:
                    target[place] = whole[look(MOVE, place), :, first : first + wide]
                else:
                    target[place] = done[place][:, first : first + wide]
            send_first(r)

        each_route(keep, c)

    def serve(c):
        if c == LAG:
            middle_tables()
        if 0 <= c - LAG < CHUNKS:
            each_route(send_second, c - LAG)
        if c == LAST_LAG:
            final_tables()
        if 0 <= c - LAST_LAG < CHUNKS:
            each_route(deliver, c - LAST_LAG)

    def exchange(t, done):
        for c in range(1, CHUNKS):

            @pl.when(t == c)
            def _():
                store(c, done)
                serve(c)

    load_first.wait()
    load_gain.wait()
    normalise_rows(cand_first, 0, 0)
    load_device.wait()
    load_slot.wait()
    own_table()
    load_bias.wait()
    load_win.wait()
    project_qkv()
    prepare_prefix()
    publish()
    load_cand.wait()

    def next_rows(t):
        normalise_rows(cand, t, pl.multiple_of(t * piece, piece))

    attend(lambda: next_rows(1))
    load_again.wait()
    load_count.wait()
    load_wout.wait()
    done = finish(0, finish_gate(), True)
    for place in range(nblk):
        whole[place] = done[place]
    done = [whole[look(ORDER_D, place)] for place in range(nblk)]
    pl.semaphore_wait(barrier, ng + nd - 2)
    store(0, done)
    send_tables()
    project_qkv()
    attend(lambda: next_rows(2))

    def step(t, carry):
        gated = finish_gate()
        project_qkv()
        done = finish(t - 1, gated)
        exchange(t - 1, done)
        attend(lambda: next_rows(jnp.minimum(t + 1, CHUNKS - 1)))
        return carry

    lax.fori_loop(2, CHUNKS, step, 0)
    last = CHUNKS - 1
    store(last, finish(last, finish_gate()))
    serve(last)
    if LAST_LAG >= CHUNKS:
        final_tables()
    waiting = max(CHUNKS - LAST_LAG, 0)
    for c in range(CHUNKS - LAG, CHUNKS):
        each_route(send_second, c)
        if waiting < c - 2:
            each_route(deliver, waiting)
            waiting += 1
    for c in range(waiting, CHUNKS):
        each_route(deliver, c)

    wait_bytes(meta_send.at[0], tab_g.at[pl.ds(1, ng - 1)])
    wait_bytes(meta_send.at[1], tab_d.at[pl.ds(1, nd - 1)])
    wait_bytes(meta_send.at[2], slot_in_1.at[pl.ds(1, nd - 1)])
    wait_bytes(meta_send.at[3], slot_in_2.at[pl.ds(1, ng - 1)])
    for r, route in enumerate(routes):
        wait_bytes(data_send.at[0, r], far(send_a[r], route[1]))
        wait_bytes(data_send.at[1, r], far(send_b[r], not route[1]))


def layer(
    ng,
    nd,
    candidates,
    prefix_keys,
    prefix_values,
    cand_count,
    prefix_len,
    dest_device,
    dest_slot,
    norm_gain,
    w_in,
    b_in,
    attn_gain,
    w_out,
):
    rows, width = candidates.shape
    prefix = prefix_keys.shape[1]
    nblk = rows // BLK
    piece = BLK // CHUNKS
    tile_rows = nblk * piece
    hbm = pl.BlockSpec(memory_space=pl.ANY)
    routes = routes_of(width)
    block = pltpu.VMEM((nblk, piece, width), BF16)
    table = pltpu.VMEM((8, 128), jnp.int32)
    out = pl.pallas_call(
        functools.partial(kernel, (ng, nd, nblk, width, prefix)),
        out_shape=jax.ShapeDtypeStruct((nblk, BLK, width), BF16),
        in_specs=[hbm] * 12,
        out_specs=pl.BlockSpec(memory_space=pltpu.VMEM),
        scratch_shapes=[
            pltpu.SMEM((1,), jnp.int32),
            pltpu.SMEM((1,), jnp.int32),
            pltpu.VMEM((1, nblk), jnp.int32),
            pltpu.VMEM((1, nblk), jnp.int32),
            pltpu.VMEM((1, width), F32),
            pltpu.VMEM((1, 4 * width), F32),
            pltpu.VMEM((1, width), F32),
            block,
            pltpu.VMEM((nblk, BLK, width), BF16),
            pltpu.VMEM((prefix, width), BF16),
            pltpu.VMEM((width, prefix), BF16),
            pltpu.VMEM((prefix, width), BF16),
            pltpu.VMEM((width, 4 * width), BF16),
            pltpu.VMEM((width, width), BF16),
            block,
            pltpu.VMEM((tile_rows, width), BF16),
            pltpu.VMEM((tile_rows, width), BF16),
            pltpu.VMEM((tile_rows, 3 * width), BF16),
            pltpu.VMEM((tile_rows, width), F32),
            table,
            pltpu.VMEM((ng, 8, 128), jnp.int32),
            pltpu.VMEM((nd, 8, 128), jnp.int32),
            table,
            table,
            pltpu.VMEM((nd, 8, 128), jnp.int32),
            pltpu.VMEM((ng, 8, 128), jnp.int32),
            table,
            pltpu.SMEM((8, 128), jnp.int32),
            pltpu.SemaphoreType.DMA((13,)),
            pltpu.SemaphoreType.DMA,
            pltpu.SemaphoreType.DMA((4,)),
            pltpu.SemaphoreType.DMA((4,)),
            pltpu.SemaphoreType.DMA((2, len(routes))),
            pltpu.SemaphoreType.DMA((2, len(routes))),
        ]
        + [pltpu.VMEM((nblk, piece, route[3]), BF16) for route in routes] * 4,
        compiler_params=pltpu.CompilerParams(
            collective_id=0, has_side_effects=True, vmem_limit_bytes=40 * 2**20
        ),
    )(
        cand_count,
        prefix_len,
        *map(
            in_hbm,
            (
                dest_device.reshape(1, nblk),
                dest_slot.reshape(1, nblk),
                norm_gain.reshape(1, width),
                b_in.reshape(1, 4 * width),
                attn_gain.reshape(1, width),
                candidates.reshape(nblk, BLK, width),
                prefix_keys[0],
                prefix_values[0],
                w_in,
                w_out,
            ),
        )
    )
    return out.reshape(rows, width)


def solution(mesh):
    spec = P(("grp", "dev"))
    wide = P(("grp", "dev"), None)
    deep = P(("grp", "dev"), None, None)
    return jax.shard_map(
        functools.partial(layer, mesh.shape["grp"], mesh.shape["dev"]),
        mesh=mesh,
        in_specs=(wide, deep, deep, spec, spec, spec, spec, P(), P(), P(), P(), P()),
        out_specs=wide,
        check_vma=False,
    )
```

```python
import functools

import jax
import jax.numpy as jnp
from jax import lax
from jax.experimental import pallas as pl
from jax.experimental.pallas import tpu as pltpu
from jax.sharding import PartitionSpec as P

HEADS = 4
BLK = 128
CHUNKS = 8
SECOND = {4: 0, 5: 1, 6: 2, 7: 3}
HALVED = (7,)
KEY_TILE = 256
AHEAD = 2
COLS = 256
MESH = pl.DeviceIdType.MESH
F32 = jnp.float32
BF16 = jnp.bfloat16
ORDER_G, ORDER_D, PICK_1, PICK_2, SLOT_1, SLOT_2, MOVE = range(7)


def in_hbm(array):
    return pltpu.with_memory_space_constraint(array, pltpu.HBM)


def log2(number):
    return number.bit_length() - 1


def lanes(shape):
    return lax.broadcasted_iota(jnp.int32, shape, 1)


def rows_of(shape):
    return lax.broadcasted_iota(jnp.int32, shape, 0)


def stack_rows(ref, count):
    tiles = []
    for first in range(0, count, 8):
        tile = jnp.full((8, 128), -1, jnp.int32)
        for step in range(first, min(first + 8, count)):
            tile = jnp.where(rows_of((8, 128)) == step - first, ref[step], tile)
        tiles.append(tile)
    return tiles[0] if len(tiles) == 1 else jnp.concatenate(tiles, axis=0)


def column(matrix, index):
    return matrix[:, index : index + 1]


def centre(matrix, width):
    average = jnp.sum(matrix, axis=-1, keepdims=True) * (1.0 / width)
    centred = matrix - average
    spread = jnp.sum(centred * centred, axis=-1, keepdims=True) * (1.0 / width)
    return centred * lax.rsqrt(spread + 1e-06)


def routes_of(width):
    routes = []
    for c in range(CHUNKS):
        if c in HALVED:
            routes += [(c, way, way * (width // 2), width // 2) for way in (0, 1)]
        else:
            routes.append((c, c % 2, 0, width))
    return routes


def half_silu(half):
    return half + half * jnp.tanh(half)


def kernel(sizes, *refs):
    ng, nd, nblk, width, prefix = sizes
    piece = BLK // CHUNKS
    tile_rows = nblk * piece
    head_dim = width // HEADS
    (
        count_hbm,
        length_hbm,
        device_hbm,
        slot_hbm,
        gain_hbm,
        bias_hbm,
        again_hbm,
        cand_hbm,
        key_hbm,
        value_hbm,
        win_hbm,
        wout_hbm,
        out_ref,
        count_ref,
        length_ref,
        device_ref,
        slot_ref,
        gain_ref,
        bias_ref,
        again_ref,
        cand_first,
        cand,
        keys,
        keys_t,
        values,
        win,
        wout,
        whole,
        nrm,
        gate,
        qkv,
        att,
        tab_own,
        tab_g,
        tab_d,
        slot_own_1,
        slot_own_2,
        slot_in_1,
        slot_in_2,
        idx_v,
        idx,
        load_sem,
        idx_sem,
        meta_send,
        meta_recv,
        data_send,
        data_recv,
        *bufs,
    ) = refs
    routes = routes_of(width)
    send_a, recv_a, send_b, recv_b = (
        bufs[len(routes) * k : len(routes) * (k + 1)] for k in range(4)
    )
    me_g = lax.axis_index("grp")
    me_d = lax.axis_index("dev")

    def at_group(step):
        return {"grp": (me_g + step) & (ng - 1), "dev": me_d}

    def at_member(step):
        return {"grp": me_g, "dev": (me_d + step) & (nd - 1)}

    (
        load_device,
        load_slot,
        load_gain,
        load_bias,
        load_again,
        load_count,
        load_length,
        load_first,
        load_win,
        load_keys,
        load_values,
        load_cand,
        load_wout,
    ) = loads = [
        pltpu.make_async_copy(src, dst, load_sem.at[k])
        for k, (src, dst) in enumerate(
            (
                (device_hbm, device_ref),
                (slot_hbm, slot_ref),
                (gain_hbm, gain_ref),
                (bias_hbm, bias_ref),
                (again_hbm, again_ref),
                (count_hbm, count_ref),
                (length_hbm, length_ref),
                (cand_hbm.at[:, pl.ds(0, piece), :], cand_first),
                (win_hbm, win),
                (key_hbm, keys),
                (value_hbm, values),
                (cand_hbm, cand),
                (wout_hbm, wout),
            )
        )
    ]
    for load in loads:
        load.start()

    barrier = pltpu.get_barrier_semaphore()

    def greet_group(step, carry):
        pl.semaphore_signal(barrier, inc=1, device_id=at_group(step), device_id_type=MESH)
        return carry

    def greet_member(step, carry):
        pl.semaphore_signal(barrier, inc=1, device_id=at_member(step), device_id_type=MESH)
        return carry

    lax.fori_loop(1, ng, greet_group, 0)
    lax.fori_loop(1, nd, greet_member, 0)

    def own_table():
        tab_own[...] = jnp.full((8, 128), -1, jnp.int32)
        code = device_ref[...] * nblk + slot_ref[...]
        tab_own[:, 0:nblk] = jnp.broadcast_to(code, (8, nblk))
        table = tab_own[...]
        device = lax.shift_right_arithmetic(table, log2(nblk))
        group = lax.shift_right_arithmetic(device, log2(nd))
        member = jnp.where(table < 0, -1, device & (nd - 1))
        lane = lanes((8, 128))
        live = lane < nblk
        want_g = jnp.where(
            live, (me_g + lax.shift_right_arithmetic(lane, 1)) & (ng - 1), -7
        )
        want_d = jnp.where(live, (me_d + lane) & (nd - 1), -7)
        low = jnp.full((8, 128), nblk - 1, jnp.int32)
        high = jnp.zeros((8, 128), jnp.int32)
        order_d = jnp.zeros((8, 128), jnp.int32)
        for i in range(nblk):
            hit_g = column(group, i) == want_g
            low = jnp.where(hit_g, jnp.minimum(low, i), low)
            high = jnp.where(hit_g, jnp.maximum(high, i), high)
            order_d = jnp.where(column(member, i) == want_d, i, order_d)
        order_g = jnp.where((lane & 1) == 0, low, high)
        move = jnp.zeros((8, 128), jnp.int32)
        for place in range(nblk):
            move = jnp.where(column(order_g, place) == order_d, place, move)
        row = rows_of((8, 128))
        idx_v[...] = jnp.where(
            row == ORDER_G,
            order_g,
            jnp.where(row == ORDER_D, order_d, jnp.where(row == MOVE, move, 0)),
        )
        tab_g[0] = table
        tab_d[0] = table

    def publish():
        copy = pltpu.make_async_copy(idx_v, idx, idx_sem)
        copy.start()
        copy.wait()

    def send_tables():
        def to_group(step, carry):
            pltpu.make_async_remote_copy(
                tab_own, tab_g.at[step], meta_send.at[0], meta_recv.at[0], at_group(step), MESH
            ).start()
            return carry

        def to_member(step, carry):
            pltpu.make_async_remote_copy(
                tab_own, tab_d.at[step], meta_send.at[1], meta_recv.at[1], at_member(step), MESH
            ).start()
            return carry

        lax.fori_loop(1, ng, to_group, 0)
        lax.fori_loop(1, nd, to_member, 0)

    def wait_bytes(sem, ref):
        pltpu.make_async_copy(ref, ref, sem).wait()

    def middle_tables():
        wait_bytes(meta_recv.at[0], tab_g.at[pl.ds(1, ng - 1)])
        wait_bytes(meta_recv.at[1], tab_d.at[pl.ds(1, nd - 1)])
        table = stack_rows(tab_g, ng)
        shape = table.shape
        device = lax.shift_right_arithmetic(table, log2(nblk))
        group = lax.shift_right_arithmetic(device, log2(nd))
        slot = table & (nblk - 1)
        lane = lanes(shape)
        mine = group == me_g
        first = jnp.min(
            jnp.where(mine, lane.astype(F32), 1000.0), axis=1, keepdims=True
        ).astype(jnp.int32)
        place = 2 * rows_of(shape) + jnp.where(lane > first, 1, 0)
        both = place * nblk + slot
        want = jnp.where(lane < nblk, me_g * nd + ((me_d + lane) & (nd - 1)), -7)
        found = jnp.zeros(shape, jnp.int32)
        for i in range(nblk):
            found = found + jnp.where(column(device, i) == want, column(both, i), 0)
        found = jnp.sum(found, axis=0, keepdims=True)
        found = jnp.broadcast_to(found, (8, 128))
        pick_1 = lax.shift_right_arithmetic(found, log2(nblk))
        slot_own_1[...] = found & (nblk - 1)
        table = stack_rows(tab_d, nd)
        shape = table.shape
        device = lax.shift_right_arithmetic(table, log2(nblk))
        both = rows_of(shape) * nblk + (table & (nblk - 1))
        lane = lanes(shape)
        want = jnp.where(
            lane < nblk,
            ((me_g + lax.shift_right_arithmetic(lane, 1)) & (ng - 1)) * nd + me_d,
            -7,
        )
        top = nd * nblk - 1
        low = jnp.full(shape, top, jnp.int32)
        high = jnp.zeros(shape, jnp.int32)
        for i in range(nblk):
            hit = column(device, i) == want
            low = jnp.where(hit, jnp.minimum(low, column(both, i)), low)
            high = jnp.where(hit, jnp.maximum(high, column(both, i)), high)
        low = jnp.broadcast_to(jnp.min(low, axis=0, keepdims=True), (8, 128))
        high = jnp.broadcast_to(jnp.max(high, axis=0, keepdims=True), (8, 128))
        found = jnp.where((lanes((8, 128)) & 1) == 0, low, high)
        pick_2 = lax.shift_right_arithmetic(found, log2(nblk))
        slot_own_2[...] = found & (nblk - 1)
        row = rows_of((8, 128))
        idx_v[...] = jnp.where(
            row == PICK_1, pick_1, jnp.where(row == PICK_2, pick_2, idx_v[...])
        )
        slot_in_1[0] = slot_own_1[...]
        slot_in_2[0] = slot_own_2[...]

        def to_member(step, carry):
            pltpu.make_async_remote_copy(
                slot_own_1, slot_in_1.at[step], meta_send.at[2], meta_recv.at[2],
                at_member(step), MESH,
            ).start()
            return carry

        def to_group(step, carry):
            pltpu.make_async_remote_copy(
                slot_own_2, slot_in_2.at[step], meta_send.at[3], meta_recv.at[3],
                at_group(step), MESH,
            ).start()
            return carry

        lax.fori_loop(1, nd, to_member, 0)
        lax.fori_loop(1, ng, to_group, 0)
        publish()

    def final_tables():
        wait_bytes(meta_recv.at[2], slot_in_1.at[pl.ds(1, nd - 1)])
        wait_bytes(meta_recv.at[3], slot_in_2.at[pl.ds(1, ng - 1)])

        def place(table, lane_of_row, number):
            lane, row = lanes(table.shape), rows_of(table.shape)
            slot = jnp.sum(
                jnp.where(lane == lane_of_row(row), table, 0).astype(F32), axis=1, keepdims=True
            ).astype(jnp.int32)
            slot = jnp.where(column(row, 0) < number, slot, -7)
            hit = jnp.where(slot == lane, lane_of_row(row), 0)
            return jnp.broadcast_to(jnp.sum(hit, axis=0, keepdims=True), (8, 128))

        table = stack_rows(slot_in_1, nd)
        slot_1 = place(table, lambda row: row, nd)
        table = stack_rows(slot_in_2, ng)
        slot_2 = place(table, lambda row: 2 * row, ng) + place(table, lambda row: 2 * row + 1, ng)
        row = rows_of((8, 128))
        idx_v[...] = jnp.where(
            row == SLOT_1, slot_1, jnp.where(row == SLOT_2, slot_2, idx_v[...])
        )
        publish()

    def look(row, lane):
        return idx[row, lane] & (nblk - 1)

    def remote(src, dst, stage, r, where):
        return pltpu.make_async_remote_copy(
            src, dst, data_send.at[stage, r], data_recv.at[stage, r], where, MESH
        )

    def to_groups(src, dst, stage, r):
        def step(number, carry):
            span = pl.ds(2 * number, 2)
            remote(src.at[span], dst.at[span], stage, r, at_group(number)).start()
            return carry

        lax.fori_loop(1, ng, step, 0, unroll=True)

    def to_members(src, dst, stage, r):
        def step(number, carry):
            remote(src.at[number], dst.at[number], stage, r, at_member(number)).start()
            return carry

        lax.fori_loop(1, nd, step, 0, unroll=True)

    def far(ref, by_group):
        return ref.at[pl.ds(2, nblk - 2)] if by_group else ref.at[pl.ds(1, nd - 1)]

    def send_first(r):
        way = routes[r][1]
        (to_groups if way else to_members)(send_a[r], recv_a[r], 0, r)

    def send_second(r):
        way = routes[r][1]
        wait_bytes(data_recv.at[0, r], far(recv_a[r], way))
        near = 1 if way else 2
        pick = PICK_1 if way else PICK_2
        for place in range(nblk):
            target = recv_b[r] if place < near else send_b[r]
            target[place] = recv_a[r][look(pick, place)]

        def step(number, carry):
            span = pl.ds(near * number, near)
            where = at_member(number) if way else at_group(number)
            remote(send_b[r].at[span], recv_b[r].at[span], 1, r, where).start()
            return carry

        lax.fori_loop(1, nblk // near, step, 0, unroll=True)

    def deliver(r):
        c, way, first, wide = routes[r]
        wait_bytes(data_recv.at[1, r], far(recv_b[r], not way))

        for s in range(nblk):
            slot = look(SLOT_1 if way else SLOT_2, s)
            out_ref[s, c * piece : (c + 1) * piece, first : first + wide] = recv_b[r][slot]

    def each_route(action, c):
        for r, route in enumerate(routes):
            if route[0] == c:
                action(r)

    def prepare_prefix():
        load_keys.wait()
        for first in range(0, prefix, KEY_TILE):
            span = slice(first, first + KEY_TILE)
            keys_t[:, span] = keys[span, :].T
        load_values.wait()
        load_length.wait()
        live = length_ref[0]
        for first in range(0, prefix, KEY_TILE):
            span = slice(first, first + KEY_TILE)
            shape = (KEY_TILE, width)
            values[span, :] = jnp.where(
                rows_of(shape) + first < live, values[span, :], jnp.zeros(shape, BF16)
            )

    score_scale = 0.5 / (head_dim**0.5)

    def order_of(t):
        by_group = t % 2 == 1
        for c in HALVED:
            by_group = jnp.logical_or(by_group, t == c)
        return jnp.where(by_group, ORDER_G, ORDER_D)

    def rows_in_order(ref, t, first_row):
        row = order_of(t)
        parts = [
            ref[look(row, place), pl.ds(first_row, piece), :] for place in range(nblk)
        ]
        return jnp.concatenate(parts, axis=0).astype(F32)

    def normalise_rows(ref, t, first_row):
        if ref is cand_first:
            x = cand_first[...].reshape(tile_rows, width).astype(F32)
        else:
            x = rows_in_order(ref, t, first_row)
        nrm[...] = (centre(x, width) * (gain_ref[...] * 0.5)).astype(BF16)

    def project(first):
        half = jnp.dot(nrm[...], win[:, first : first + COLS], preferred_element_type=F32)
        return half_silu(half + bias_ref[:, first : first + COLS] * 0.5)

    def project_qkv():
        for first in range(width, 4 * width, COLS):
            act = project(first)
            if 2 * width <= first < 3 * width:
                act = act * score_scale
            qkv[:, first - width : first - width + COLS] = act.astype(BF16)

    def attend(following):
        for first in range(0, width, COLS):
            gate[:, first : first + COLS] = project(first).astype(BF16)
        tiles = [(h, first) for h in range(HEADS) for first in range(0, prefix, KEY_TILE)]

        def part_of(group, h):
            first = group * width + h * head_dim
            return qkv[:, first : first + head_dim]

        def score(tile):
            h, first = tile
            cols = slice(h * head_dim, (h + 1) * head_dim)
            return jnp.dot(
                part_of(1, h), keys_t[cols, first : first + KEY_TILE], preferred_element_type=F32
            )

        ahead = [score(tile) for tile in tiles[:AHEAD]]
        totals = [None] * HEADS
        for number, (h, first) in enumerate(tiles):
            half = ahead.pop(0)
            if number + AHEAD < len(tiles):
                ahead.append(score(tiles[number + AHEAD]))
            cols = slice(h * head_dim, (h + 1) * head_dim)
            weights = half_silu(half).astype(BF16)
            term = jnp.dot(
                weights, values[first : first + KEY_TILE, cols], preferred_element_type=F32
            )
            totals[h] = term if totals[h] is None else totals[h] + term
            if first + KEY_TILE == prefix:
                own = jnp.sum(
                    part_of(1, h).astype(F32) * part_of(2, h).astype(F32), axis=-1, keepdims=True
                )
                own = half_silu(own).astype(BF16).astype(F32)
                att[:, cols] = totals[h] + own * part_of(0, h).astype(F32)
                if h == 0 and following is not None:
                    following()

    def finish_gate():
        return (
            centre(att[...], width) * again_ref[...] * gate[...].astype(F32)
        ).astype(BF16)

    def finish(t, gated, stored_order=False):
        first_row = t * piece if stored_order else pl.multiple_of(t * piece, piece)
        delta = jnp.dot(gated, wout[...], preferred_element_type=F32)
        row = order_of(t)
        count = count_ref[0]
        done = []
        for place in range(nblk):
            block = place if stored_order else look(row, place)
            x = cand[block, pl.ds(first_row, piece), :].astype(F32)
            x = x + delta[place * piece : (place + 1) * piece, :]
            live = rows_of((piece, width)) + (block * BLK + first_row) < count
            done.append(jnp.where(live, x, 0.0).astype(BF16))
        return done

    def store(c, done):
        if c in HALVED:
            for place in range(nblk):
                whole[place] = done[place]

        def keep(r):
            way, first, wide = routes[r][1:]
            near = 2 if way else 1
            for place in range(nblk):
                target = recv_a[r] if place < near else send_a[r]
                if c in HALVED and not way:
                    target[place] = whole[look(MOVE, place), :, first : first + wide]
                else:
                    target[place] = done[place][:, first : first + wide]
            send_first(r)

        each_route(keep, c)

    def serve(c):
        if c == min(SECOND):
            middle_tables()
        if c in SECOND:
            each_route(send_second, SECOND[c])

    def exchange(t, done):
        for c in range(1, CHUNKS):

            @pl.when(t == c)
            def _():
                store(c, done)
                serve(c)

    load_first.wait()
    load_gain.wait()
    normalise_rows(cand_first, 0, 0)
    load_device.wait()
    load_slot.wait()
    own_table()
    load_bias.wait()
    load_win.wait()
    project_qkv()
    prepare_prefix()
    publish()
    load_cand.wait()

    def next_rows(t):
        normalise_rows(cand, t, pl.multiple_of(t * piece, piece))

    attend(lambda: next_rows(1))
    load_again.wait()
    load_count.wait()
    load_wout.wait()
    done = finish(0, finish_gate(), True)
    for place in range(nblk):
        whole[place] = done[place]
    done = [whole[look(ORDER_D, place)] for place in range(nblk)]
    pl.semaphore_wait(barrier, ng + nd - 2)
    store(0, done)
    send_tables()
    project_qkv()
    attend(lambda: next_rows(2))

    def step(t, carry):
        gated = finish_gate()
        project_qkv()
        done = finish(t - 1, gated)
        exchange(t - 1, done)
        attend(lambda: next_rows(jnp.minimum(t + 1, CHUNKS - 1)))
        return carry

    lax.fori_loop(2, CHUNKS, step, 0)
    last = CHUNKS - 1
    store(last, finish(last, finish_gate()))
    serve(last)
    for c in range(len(SECOND), last):
        each_route(send_second, c)
    each_route(send_second, last)
    final_tables()
    for c in range(CHUNKS):
        each_route(deliver, c)

    wait_bytes(meta_send.at[0], tab_g.at[pl.ds(1, ng - 1)])
    wait_bytes(meta_send.at[1], tab_d.at[pl.ds(1, nd - 1)])
    wait_bytes(meta_send.at[2], slot_in_1.at[pl.ds(1, nd - 1)])
    wait_bytes(meta_send.at[3], slot_in_2.at[pl.ds(1, ng - 1)])
    for r, route in enumerate(routes):
        wait_bytes(data_send.at[0, r], far(send_a[r], route[1]))
        wait_bytes(data_send.at[1, r], far(send_b[r], not route[1]))


def layer(
    ng,
    nd,
    candidates,
    prefix_keys,
    prefix_values,
    cand_count,
    prefix_len,
    dest_device,
    dest_slot,
    norm_gain,
    w_in,
    b_in,
    attn_gain,
    w_out,
):
    rows, width = candidates.shape
    prefix = prefix_keys.shape[1]
    nblk = rows // BLK
    piece = BLK // CHUNKS
    tile_rows = nblk * piece
    hbm = pl.BlockSpec(memory_space=pl.ANY)
    routes = routes_of(width)
    block = pltpu.VMEM((nblk, piece, width), BF16)
    table = pltpu.VMEM((8, 128), jnp.int32)
    out = pl.pallas_call(
        functools.partial(kernel, (ng, nd, nblk, width, prefix)),
        out_shape=jax.ShapeDtypeStruct((nblk, BLK, width), BF16),
        in_specs=[hbm] * 12,
        out_specs=pl.BlockSpec(memory_space=pltpu.VMEM),
        scratch_shapes=[
            pltpu.SMEM((1,), jnp.int32),
            pltpu.SMEM((1,), jnp.int32),
            pltpu.VMEM((1, nblk), jnp.int32),
            pltpu.VMEM((1, nblk), jnp.int32),
            pltpu.VMEM((1, width), F32),
            pltpu.VMEM((1, 4 * width), F32),
            pltpu.VMEM((1, width), F32),
            block,
            pltpu.VMEM((nblk, BLK, width), BF16),
            pltpu.VMEM((prefix, width), BF16),
            pltpu.VMEM((width, prefix), BF16),
            pltpu.VMEM((prefix, width), BF16),
            pltpu.VMEM((width, 4 * width), BF16),
            pltpu.VMEM((width, width), BF16),
            block,
            pltpu.VMEM((tile_rows, width), BF16),
            pltpu.VMEM((tile_rows, width), BF16),
            pltpu.VMEM((tile_rows, 3 * width), BF16),
            pltpu.VMEM((tile_rows, width), F32),
            table,
            pltpu.VMEM((ng, 8, 128), jnp.int32),
            pltpu.VMEM((nd, 8, 128), jnp.int32),
            table,
            table,
            pltpu.VMEM((nd, 8, 128), jnp.int32),
            pltpu.VMEM((ng, 8, 128), jnp.int32),
            table,
            pltpu.SMEM((8, 128), jnp.int32),
            pltpu.SemaphoreType.DMA((13,)),
            pltpu.SemaphoreType.DMA,
            pltpu.SemaphoreType.DMA((4,)),
            pltpu.SemaphoreType.DMA((4,)),
            pltpu.SemaphoreType.DMA((2, len(routes))),
            pltpu.SemaphoreType.DMA((2, len(routes))),
        ]
        + [pltpu.VMEM((nblk, piece, route[3]), BF16) for route in routes] * 4,
        compiler_params=pltpu.CompilerParams(
            collective_id=0, has_side_effects=True, vmem_limit_bytes=40 * 2**20
        ),
    )(
        cand_count,
        prefix_len,
        *map(
            in_hbm,
            (
                dest_device.reshape(1, nblk),
                dest_slot.reshape(1, nblk),
                norm_gain.reshape(1, width),
                b_in.reshape(1, 4 * width),
                attn_gain.reshape(1, width),
                candidates.reshape(nblk, BLK, width),
                prefix_keys[0],
                prefix_values[0],
                w_in,
                w_out,
            ),
        )
    )
    return out.reshape(rows, width)


def solution(mesh):
    spec = P(("grp", "dev"))
    wide = P(("grp", "dev"), None)
    deep = P(("grp", "dev"), None, None)
    return jax.shard_map(
        functools.partial(layer, mesh.shape["grp"], mesh.shape["dev"]),
        mesh=mesh,
        in_specs=(wide, deep, deep, spec, spec, spec, spec, P(), P(), P(), P(), P()),
        out_specs=wide,
        check_vma=False,
    )
```

```python
import functools

import jax
import jax.numpy as jnp
from jax import lax
from jax.experimental import pallas as pl
from jax.experimental.pallas import tpu as pltpu
from jax.sharding import PartitionSpec as P

HEADS = 4
BLK = 128
CHUNKS = 8
SECOND = {4: 0, 5: 1, 6: 2, 7: 3}
HALVED = (7,)
KEY_TILE = 256
AHEAD = 2
COLS = 256
MESH = pl.DeviceIdType.MESH
F32 = jnp.float32
BF16 = jnp.bfloat16
ORDER_G, ORDER_D, PICK_1, PICK_2, SLOT_1, SLOT_2, MOVE = range(7)


def in_hbm(array):
    return pltpu.with_memory_space_constraint(array, pltpu.HBM)


def log2(number):
    return number.bit_length() - 1


def lanes(shape):
    return lax.broadcasted_iota(jnp.int32, shape, 1)


def rows_of(shape):
    return lax.broadcasted_iota(jnp.int32, shape, 0)


def stack_rows(ref, count):
    tiles = []
    for first in range(0, count, 8):
        tile = jnp.full((8, 128), -1, jnp.int32)
        for step in range(first, min(first + 8, count)):
            tile = jnp.where(rows_of((8, 128)) == step - first, ref[step], tile)
        tiles.append(tile)
    return tiles[0] if len(tiles) == 1 else jnp.concatenate(tiles, axis=0)


def column(matrix, index):
    return matrix[:, index : index + 1]


def centre(matrix, width):
    average = jnp.sum(matrix, axis=-1, keepdims=True) * (1.0 / width)
    centred = matrix - average
    spread = jnp.sum(centred * centred, axis=-1, keepdims=True) * (1.0 / width)
    return centred * lax.rsqrt(spread + 1e-06)


def routes_of(width):
    routes = []
    for c in range(CHUNKS):
        if c in HALVED:
            routes += [(c, way, way * (width // 2), width // 2) for way in (0, 1)]
        else:
            routes.append((c, c % 2, 0, width))
    return routes


def half_silu(half):
    return half + half * jnp.tanh(half)


def kernel(sizes, *refs):
    ng, nd, nblk, width, prefix = sizes
    piece = BLK // CHUNKS
    tile_rows = nblk * piece
    head_dim = width // HEADS
    (
        count_hbm,
        length_hbm,
        device_hbm,
        slot_hbm,
        gain_hbm,
        bias_hbm,
        again_hbm,
        cand_hbm,
        key_hbm,
        value_hbm,
        win_hbm,
        wout_hbm,
        out_ref,
        count_ref,
        length_ref,
        device_ref,
        slot_ref,
        gain_ref,
        bias_ref,
        again_ref,
        cand_first,
        cand,
        keys,
        keys_t,
        values,
        win,
        wout,
        whole,
        nrm,
        gate,
        qkv,
        att,
        tab_own,
        tab_g,
        tab_d,
        slot_own_1,
        slot_own_2,
        slot_in_1,
        slot_in_2,
        idx_v,
        idx,
        idx_mid,
        load_sem,
        idx_sem,
        meta_send,
        meta_recv,
        data_send,
        data_recv,
        *bufs,
    ) = refs
    routes = routes_of(width)
    send_a, recv_a, send_b, recv_b = (
        bufs[len(routes) * k : len(routes) * (k + 1)] for k in range(4)
    )
    me_g = lax.axis_index("grp")
    me_d = lax.axis_index("dev")

    def at_group(step):
        return {"grp": (me_g + step) & (ng - 1), "dev": me_d}

    def at_member(step):
        return {"grp": me_g, "dev": (me_d + step) & (nd - 1)}

    (
        load_device,
        load_slot,
        load_gain,
        load_bias,
        load_again,
        load_count,
        load_length,
        load_first,
        load_win,
        load_keys,
        load_values,
        load_cand,
        load_wout,
    ) = loads = [
        pltpu.make_async_copy(src, dst, load_sem.at[k])
        for k, (src, dst) in enumerate(
            (
                (device_hbm, device_ref),
                (slot_hbm, slot_ref),
                (gain_hbm, gain_ref),
                (bias_hbm, bias_ref),
                (again_hbm, again_ref),
                (count_hbm, count_ref),
                (length_hbm, length_ref),
                (cand_hbm.at[:, pl.ds(0, piece), :], cand_first),
                (win_hbm, win),
                (key_hbm, keys),
                (value_hbm, values),
                (cand_hbm, cand),
                (wout_hbm, wout),
            )
        )
    ]
    for load in loads:
        load.start()

    barrier = pltpu.get_barrier_semaphore()

    def greet_group(step, carry):
        pl.semaphore_signal(barrier, inc=1, device_id=at_group(step), device_id_type=MESH)
        return carry

    def greet_member(step, carry):
        pl.semaphore_signal(barrier, inc=1, device_id=at_member(step), device_id_type=MESH)
        return carry

    lax.fori_loop(1, ng, greet_group, 0)
    lax.fori_loop(1, nd, greet_member, 0)

    def own_table():
        tab_own[...] = jnp.full((8, 128), -1, jnp.int32)
        code = device_ref[...] * nblk + slot_ref[...]
        tab_own[:, 0:nblk] = jnp.broadcast_to(code, (8, nblk))
        table = tab_own[...]
        device = lax.shift_right_arithmetic(table, log2(nblk))
        group = lax.shift_right_arithmetic(device, log2(nd))
        member = jnp.where(table < 0, -1, device & (nd - 1))
        lane = lanes((8, 128))
        live = lane < nblk
        want_g = jnp.where(
            live, (me_g + lax.shift_right_arithmetic(lane, 1)) & (ng - 1), -7
        )
        want_d = jnp.where(live, (me_d + lane) & (nd - 1), -7)
        low = jnp.full((8, 128), nblk - 1, jnp.int32)
        high = jnp.zeros((8, 128), jnp.int32)
        order_d = jnp.zeros((8, 128), jnp.int32)
        for i in range(nblk):
            hit_g = column(group, i) == want_g
            low = jnp.where(hit_g, jnp.minimum(low, i), low)
            high = jnp.where(hit_g, jnp.maximum(high, i), high)
            order_d = jnp.where(column(member, i) == want_d, i, order_d)
        order_g = jnp.where((lane & 1) == 0, low, high)
        move = jnp.zeros((8, 128), jnp.int32)
        for place in range(nblk):
            move = jnp.where(column(order_g, place) == order_d, place, move)
        row = rows_of((8, 128))
        idx_v[...] = jnp.where(
            row == ORDER_G,
            order_g,
            jnp.where(row == ORDER_D, order_d, jnp.where(row == MOVE, move, 0)),
        )
        tab_g[0] = table
        tab_d[0] = table

    def publish():
        copy = pltpu.make_async_copy(idx_v, idx, idx_sem)
        copy.start()
        copy.wait()

    def send_tables():
        def to_group(step, carry):
            pltpu.make_async_remote_copy(
                tab_own, tab_g.at[step], meta_send.at[0], meta_recv.at[0], at_group(step), MESH
            ).start()
            return carry

        def to_member(step, carry):
            pltpu.make_async_remote_copy(
                tab_own, tab_d.at[step], meta_send.at[1], meta_recv.at[1], at_member(step), MESH
            ).start()
            return carry

        lax.fori_loop(1, ng, to_group, 0)
        lax.fori_loop(1, nd, to_member, 0)

    def wait_bytes(sem, ref):
        pltpu.make_async_copy(ref, ref, sem).wait()

    def middle_tables():
        wait_bytes(meta_recv.at[0], tab_g.at[pl.ds(1, ng - 1)])
        wait_bytes(meta_recv.at[1], tab_d.at[pl.ds(1, nd - 1)])
        table = stack_rows(tab_g, ng)
        shape = table.shape
        device = lax.shift_right_arithmetic(table, log2(nblk))
        group = lax.shift_right_arithmetic(device, log2(nd))
        slot = table & (nblk - 1)
        lane = lanes(shape)
        mine = group == me_g
        first = jnp.min(
            jnp.where(mine, lane.astype(F32), 1000.0), axis=1, keepdims=True
        ).astype(jnp.int32)
        place = 2 * rows_of(shape) + jnp.where(lane > first, 1, 0)
        both = place * nblk + slot
        want = jnp.where(lane < nblk, me_g * nd + ((me_d + lane) & (nd - 1)), -7)
        found = jnp.zeros(shape, jnp.int32)
        for i in range(nblk):
            found = found + jnp.where(column(device, i) == want, column(both, i), 0)
        found = jnp.sum(found, axis=0, keepdims=True)
        found = jnp.broadcast_to(found, (8, 128))
        pick_1 = lax.shift_right_arithmetic(found, log2(nblk))
        slot_own_1[...] = found & (nblk - 1)
        table = stack_rows(tab_d, nd)
        shape = table.shape
        device = lax.shift_right_arithmetic(table, log2(nblk))
        both = rows_of(shape) * nblk + (table & (nblk - 1))
        lane = lanes(shape)
        want = jnp.where(
            lane < nblk,
            ((me_g + lax.shift_right_arithmetic(lane, 1)) & (ng - 1)) * nd + me_d,
            -7,
        )
        top = nd * nblk - 1
        low = jnp.full(shape, top, jnp.int32)
        high = jnp.zeros(shape, jnp.int32)
        for i in range(nblk):
            hit = column(device, i) == want
            low = jnp.where(hit, jnp.minimum(low, column(both, i)), low)
            high = jnp.where(hit, jnp.maximum(high, column(both, i)), high)
        low = jnp.broadcast_to(jnp.min(low, axis=0, keepdims=True), (8, 128))
        high = jnp.broadcast_to(jnp.max(high, axis=0, keepdims=True), (8, 128))
        found = jnp.where((lanes((8, 128)) & 1) == 0, low, high)
        pick_2 = lax.shift_right_arithmetic(found, log2(nblk))
        slot_own_2[...] = found & (nblk - 1)
        row = rows_of((8, 128))
        idx_v[...] = jnp.where(
            row == PICK_1, pick_1, jnp.where(row == PICK_2, pick_2, idx_v[...])
        )
        slot_in_1[0] = slot_own_1[...]
        slot_in_2[0] = slot_own_2[...]

        def to_member(step, carry):
            pltpu.make_async_remote_copy(
                slot_own_1, slot_in_1.at[step], meta_send.at[2], meta_recv.at[2],
                at_member(step), MESH,
            ).start()
            return carry

        def to_group(step, carry):
            pltpu.make_async_remote_copy(
                slot_own_2, slot_in_2.at[step], meta_send.at[3], meta_recv.at[3],
                at_group(step), MESH,
            ).start()
            return carry

        lax.fori_loop(1, nd, to_member, 0)
        lax.fori_loop(1, ng, to_group, 0)
        pltpu.make_async_copy(idx_v, idx_mid, idx_sem).start()

    def final_tables():
        wait_bytes(meta_recv.at[2], slot_in_1.at[pl.ds(1, nd - 1)])
        wait_bytes(meta_recv.at[3], slot_in_2.at[pl.ds(1, ng - 1)])

        def place(table, lane_of_row, number):
            lane, row = lanes(table.shape), rows_of(table.shape)
            slot = jnp.sum(
                jnp.where(lane == lane_of_row(row), table, 0).astype(F32), axis=1, keepdims=True
            ).astype(jnp.int32)
            slot = jnp.where(column(row, 0) < number, slot, -7)
            hit = jnp.where(slot == lane, lane_of_row(row), 0)
            return jnp.broadcast_to(jnp.sum(hit, axis=0, keepdims=True), (8, 128))

        table = stack_rows(slot_in_1, nd)
        slot_1 = place(table, lambda row: row, nd)
        table = stack_rows(slot_in_2, ng)
        slot_2 = place(table, lambda row: 2 * row, ng) + place(table, lambda row: 2 * row + 1, ng)
        row = rows_of((8, 128))
        idx_v[...] = jnp.where(
            row == SLOT_1, slot_1, jnp.where(row == SLOT_2, slot_2, idx_v[...])
        )
        publish()

    def look(row, lane):
        middle = isinstance(row, int) and row in (PICK_1, PICK_2)
        table = idx_mid if middle else idx
        return table[row, lane] & (nblk - 1)

    def remote(src, dst, stage, r, where):
        return pltpu.make_async_remote_copy(
            src, dst, data_send.at[stage, r], data_recv.at[stage, r], where, MESH
        )

    def to_groups(src, dst, stage, r):
        def step(number, carry):
            span = pl.ds(2 * number, 2)
            remote(src.at[span], dst.at[span], stage, r, at_group(number)).start()
            return carry

        lax.fori_loop(1, ng, step, 0, unroll=True)

    def to_members(src, dst, stage, r):
        def step(number, carry):
            remote(src.at[number], dst.at[number], stage, r, at_member(number)).start()
            return carry

        lax.fori_loop(1, nd, step, 0, unroll=True)

    def far(ref, by_group):
        return ref.at[pl.ds(2, nblk - 2)] if by_group else ref.at[pl.ds(1, nd - 1)]

    def send_first(r):
        way = routes[r][1]
        (to_groups if way else to_members)(send_a[r], recv_a[r], 0, r)

    def send_second(r):
        way = routes[r][1]
        wait_bytes(data_recv.at[0, r], far(recv_a[r], way))
        near = 1 if way else 2
        pick = PICK_1 if way else PICK_2
        for place in range(nblk):
            target = recv_b[r] if place < near else send_b[r]
            target[place] = recv_a[r][look(pick, place)]

        def step(number, carry):
            span = pl.ds(near * number, near)
            where = at_member(number) if way else at_group(number)
            remote(send_b[r].at[span], recv_b[r].at[span], 1, r, where).start()
            return carry

        lax.fori_loop(1, nblk // near, step, 0, unroll=True)

    def deliver(r):
        c, way, first, wide = routes[r]
        wait_bytes(data_recv.at[1, r], far(recv_b[r], not way))

        for s in range(nblk):
            slot = look(SLOT_1 if way else SLOT_2, s)
            out_ref[s, c * piece : (c + 1) * piece, first : first + wide] = recv_b[r][slot]

    def each_route(action, c):
        for r, route in enumerate(routes):
            if route[0] == c:
                action(r)

    def prepare_prefix():
        load_keys.wait()
        for first in range(0, prefix, KEY_TILE):
            span = slice(first, first + KEY_TILE)
            keys_t[:, span] = keys[span, :].T
        load_values.wait()
        load_length.wait()
        live = length_ref[0]
        for first in range(0, prefix, KEY_TILE):
            span = slice(first, first + KEY_TILE)
            shape = (KEY_TILE, width)
            values[span, :] = jnp.where(
                rows_of(shape) + first < live, values[span, :], jnp.zeros(shape, BF16)
            )

    score_scale = 0.5 / (head_dim**0.5)

    def order_of(t):
        by_group = t % 2 == 1
        for c in HALVED:
            by_group = jnp.logical_or(by_group, t == c)
        return jnp.where(by_group, ORDER_G, ORDER_D)

    def rows_in_order(ref, t, first_row):
        row = order_of(t)
        parts = [
            ref[look(row, place), pl.ds(first_row, piece), :] for place in range(nblk)
        ]
        return jnp.concatenate(parts, axis=0).astype(F32)

    def normalise_rows(ref, t, first_row):
        if ref is cand_first:
            x = cand_first[...].reshape(tile_rows, width).astype(F32)
        else:
            x = rows_in_order(ref, t, first_row)
        nrm[...] = (centre(x, width) * (gain_ref[...] * 0.5)).astype(BF16)

    def project(first):
        half = jnp.dot(nrm[...], win[:, first : first + COLS], preferred_element_type=F32)
        return half_silu(half + bias_ref[:, first : first + COLS] * 0.5)

    def project_qkv():
        for first in range(width, 4 * width, COLS):
            act = project(first)
            if 2 * width <= first < 3 * width:
                act = act * score_scale
            qkv[:, first - width : first - width + COLS] = act.astype(BF16)

    def attend(following):
        for first in range(0, width, COLS):
            gate[:, first : first + COLS] = project(first).astype(BF16)
        tiles = [(h, first) for h in range(HEADS) for first in range(0, prefix, KEY_TILE)]

        def part_of(group, h):
            first = group * width + h * head_dim
            return qkv[:, first : first + head_dim]

        def score(tile):
            h, first = tile
            cols = slice(h * head_dim, (h + 1) * head_dim)
            return jnp.dot(
                part_of(1, h), keys_t[cols, first : first + KEY_TILE], preferred_element_type=F32
            )

        ahead = [score(tile) for tile in tiles[:AHEAD]]
        totals = [None] * HEADS
        for number, (h, first) in enumerate(tiles):
            half = ahead.pop(0)
            if number + AHEAD < len(tiles):
                ahead.append(score(tiles[number + AHEAD]))
            cols = slice(h * head_dim, (h + 1) * head_dim)
            weights = half_silu(half).astype(BF16)
            term = jnp.dot(
                weights, values[first : first + KEY_TILE, cols], preferred_element_type=F32
            )
            totals[h] = term if totals[h] is None else totals[h] + term
            if first + KEY_TILE == prefix:
                own = jnp.sum(
                    part_of(1, h).astype(F32) * part_of(2, h).astype(F32), axis=-1, keepdims=True
                )
                own = half_silu(own).astype(BF16).astype(F32)
                att[:, cols] = totals[h] + own * part_of(0, h).astype(F32)
                if h == 0 and following is not None:
                    following()

    def finish_gate():
        return (
            centre(att[...], width) * again_ref[...] * gate[...].astype(F32)
        ).astype(BF16)

    def finish(t, gated, stored_order=False):
        first_row = t * piece if stored_order else pl.multiple_of(t * piece, piece)
        delta = jnp.dot(gated, wout[...], preferred_element_type=F32)
        row = order_of(t)
        count = count_ref[0]
        done = []
        for place in range(nblk):
            block = place if stored_order else look(row, place)
            x = cand[block, pl.ds(first_row, piece), :].astype(F32)
            x = x + delta[place * piece : (place + 1) * piece, :]
            live = rows_of((piece, width)) + (block * BLK + first_row) < count
            done.append(jnp.where(live, x, 0.0).astype(BF16))
        return done

    def store(c, done):
        if c in HALVED:
            for place in range(nblk):
                whole[place] = done[place]

        def keep(r):
            way, first, wide = routes[r][1:]
            near = 2 if way else 1
            for place in range(nblk):
                target = recv_a[r] if place < near else send_a[r]
                if c in HALVED and not way:
                    target[place] = whole[look(MOVE, place), :, first : first + wide]
                else:
                    target[place] = done[place][:, first : first + wide]
            send_first(r)

        each_route(keep, c)

    def serve(c):
        if c == min(SECOND) - 1:
            middle_tables()
        if c == min(SECOND):
            pltpu.make_async_copy(idx_v, idx_mid, idx_sem).wait()
        if c in SECOND:
            each_route(send_second, SECOND[c])

    def exchange(t, done):
        for c in range(1, CHUNKS):

            @pl.when(t == c)
            def _():
                store(c, done)
                serve(c)

    load_first.wait()
    load_gain.wait()
    normalise_rows(cand_first, 0, 0)
    load_device.wait()
    load_slot.wait()
    own_table()
    load_bias.wait()
    load_win.wait()
    project_qkv()
    prepare_prefix()
    publish()
    load_cand.wait()

    def next_rows(t):
        normalise_rows(cand, t, pl.multiple_of(t * piece, piece))

    attend(lambda: next_rows(1))
    load_again.wait()
    load_count.wait()
    load_wout.wait()
    done = finish(0, finish_gate(), True)
    for place in range(nblk):
        whole[place] = done[place]
    done = [whole[look(ORDER_D, place)] for place in range(nblk)]
    pl.semaphore_wait(barrier, ng + nd - 2)
    store(0, done)
    send_tables()
    project_qkv()
    attend(lambda: next_rows(2))

    def step(t, carry):
        gated = finish_gate()
        project_qkv()
        done = finish(t - 1, gated)
        exchange(t - 1, done)
        attend(lambda: next_rows(jnp.minimum(t + 1, CHUNKS - 1)))
        return carry

    lax.fori_loop(2, CHUNKS, step, 0)
    last = CHUNKS - 1
    store(last, finish(last, finish_gate()))
    serve(last)
    for c in range(len(SECOND), last):
        each_route(send_second, c)
    each_route(send_second, last)
    final_tables()
    for c in range(CHUNKS):
        each_route(deliver, c)

    wait_bytes(meta_send.at[0], tab_g.at[pl.ds(1, ng - 1)])
    wait_bytes(meta_send.at[1], tab_d.at[pl.ds(1, nd - 1)])
    wait_bytes(meta_send.at[2], slot_in_1.at[pl.ds(1, nd - 1)])
    wait_bytes(meta_send.at[3], slot_in_2.at[pl.ds(1, ng - 1)])
    for r, route in enumerate(routes):
        wait_bytes(data_send.at[0, r], far(send_a[r], route[1]))
        wait_bytes(data_send.at[1, r], far(send_b[r], not route[1]))


def layer(
    ng,
    nd,
    candidates,
    prefix_keys,
    prefix_values,
    cand_count,
    prefix_len,
    dest_device,
    dest_slot,
    norm_gain,
    w_in,
    b_in,
    attn_gain,
    w_out,
):
    rows, width = candidates.shape
    prefix = prefix_keys.shape[1]
    nblk = rows // BLK
    piece = BLK // CHUNKS
    tile_rows = nblk * piece
    hbm = pl.BlockSpec(memory_space=pl.ANY)
    routes = routes_of(width)
    block = pltpu.VMEM((nblk, piece, width), BF16)
    table = pltpu.VMEM((8, 128), jnp.int32)
    out = pl.pallas_call(
        functools.partial(kernel, (ng, nd, nblk, width, prefix)),
        out_shape=jax.ShapeDtypeStruct((nblk, BLK, width), BF16),
        in_specs=[hbm] * 12,
        out_specs=pl.BlockSpec(memory_space=pltpu.VMEM),
        scratch_shapes=[
            pltpu.SMEM((1,), jnp.int32),
            pltpu.SMEM((1,), jnp.int32),
            pltpu.VMEM((1, nblk), jnp.int32),
            pltpu.VMEM((1, nblk), jnp.int32),
            pltpu.VMEM((1, width), F32),
            pltpu.VMEM((1, 4 * width), F32),
            pltpu.VMEM((1, width), F32),
            block,
            pltpu.VMEM((nblk, BLK, width), BF16),
            pltpu.VMEM((prefix, width), BF16),
            pltpu.VMEM((width, prefix), BF16),
            pltpu.VMEM((prefix, width), BF16),
            pltpu.VMEM((width, 4 * width), BF16),
            pltpu.VMEM((width, width), BF16),
            block,
            pltpu.VMEM((tile_rows, width), BF16),
            pltpu.VMEM((tile_rows, width), BF16),
            pltpu.VMEM((tile_rows, 3 * width), BF16),
            pltpu.VMEM((tile_rows, width), F32),
            table,
            pltpu.VMEM((ng, 8, 128), jnp.int32),
            pltpu.VMEM((nd, 8, 128), jnp.int32),
            table,
            table,
            pltpu.VMEM((nd, 8, 128), jnp.int32),
            pltpu.VMEM((ng, 8, 128), jnp.int32),
            table,
            pltpu.SMEM((8, 128), jnp.int32),
            pltpu.SMEM((8, 128), jnp.int32),
            pltpu.SemaphoreType.DMA((13,)),
            pltpu.SemaphoreType.DMA,
            pltpu.SemaphoreType.DMA((4,)),
            pltpu.SemaphoreType.DMA((4,)),
            pltpu.SemaphoreType.DMA((2, len(routes))),
            pltpu.SemaphoreType.DMA((2, len(routes))),
        ]
        + [pltpu.VMEM((nblk, piece, route[3]), BF16) for route in routes] * 4,
        compiler_params=pltpu.CompilerParams(
            collective_id=0, has_side_effects=True, vmem_limit_bytes=40 * 2**20
        ),
    )(
        cand_count,
        prefix_len,
        *map(
            in_hbm,
            (
                dest_device.reshape(1, nblk),
                dest_slot.reshape(1, nblk),
                norm_gain.reshape(1, width),
                b_in.reshape(1, 4 * width),
                attn_gain.reshape(1, width),
                candidates.reshape(nblk, BLK, width),
                prefix_keys[0],
                prefix_values[0],
                w_in,
                w_out,
            ),
        )
    )
    return out.reshape(rows, width)


def solution(mesh):
    spec = P(("grp", "dev"))
    wide = P(("grp", "dev"), None)
    deep = P(("grp", "dev"), None, None)
    return jax.shard_map(
        functools.partial(layer, mesh.shape["grp"], mesh.shape["dev"]),
        mesh=mesh,
        in_specs=(wide, deep, deep, spec, spec, spec, spec, P(), P(), P(), P(), P()),
        out_specs=wide,
        check_vma=False,
    )
```
